32 devices in a mesh: seq: 16 (over z, y, x), tp: 2 (over core).
Axes of the slice: x: 2, y: 2, z: 4, core: 2. Of those that a mesh axis runs over, the one named last changes fastest.
Arguments:
- img: bfloat16 [4, 512, 3072], P(None, 'seq', 'tp'), may hold values from -6 to 6
- txt: bfloat16 [4, 64, 3072], P(None, 'seq', 'tp'), may hold values from -6 to 6
- prev_mod: bfloat16 [4, 512, 3072], P(None, 'seq', 'tp'), may hold values from -47 to 47
- cache: float32 [4, 512, 3072], P(None, 'seq', 'tp'), may hold values from -6 to 6
- modulation: bfloat16 [3, 4, 3072], P(None, None, 'tp'), may hold values from -4 to 4
- w_qkv: bfloat16 [3072, 3, 2048], P('seq', None, 'tp'), may hold values from -1 to 1, as said below
- qk_gain: float32 [2, 2048], P(None, 'tp'), may hold values from 0.5 to 6, as said below
- output_weight: bfloat16 [2048, 3072], P('tp'), may hold values from -0.1875 to 0.1875
- text_len: int32 [4], replicated, may hold values from 1 to 64
- refresh: int32 [4], replicated, may hold values from 0 to 1, as said below
Outputs:
- out_img: float32 [4, 512, 3072], P(None, 'seq', 'tp')
- new_cache: float32 [4, 512, 3072], P(None, 'seq', 'tp')
- rel_l1: float32 [4], replicated
The draws below stay inside these ranges and needn't reach their ends.
Inputs may be any that keep to these rules, and one draw needn't show every extreme that they name: `refresh`: at least one sequence has flag 1 and at least one has flag 0. `w_qkv`: entries of spread about one over the square root of 3072. `qk_gain`: positive.
All inputs are finite; a program needn't handle non-finite values.
Results may differ from the reference program's by a relative error of at most 0.013.
The reference program's roundings to bfloat16 on the way count: a program that leaves them out, or rounds other values in their place, can miss the bound.
Values may be sent and summed in bfloat16 or wider, within the bound.
A program may use at most 128 MiB of HBM per device.

```python
import math
import jax
import jax.numpy as jnp
from jax import lax

D = 3072
HEADS = 16
HD = 128
BATCH = 4
IMG = 512
TXT = 64


def draw_w_qkv(key, part):
    limit = 6.0 / math.sqrt(D)
    base = jnp.clip(jax.random.normal(key, (D, 3, HEADS * HD), jnp.float32) / math.sqrt(D), -limit, limit)
    return base.astype(jnp.bfloat16)


def draw_qk_gain(key, part):
    logs = jax.random.uniform(key, (2, HEADS * HD), jnp.float32, math.log(0.5), math.log(3.0))
    return jnp.exp(logs)


def draw_prev_mod(key, part):
    first = jax.random.fold_in(key, 11)
    second = jax.random.fold_in(key, 12)
    third = jax.random.fold_in(key, 13)
    base = jnp.clip(jax.random.normal(first, (BATCH, IMG, D), jnp.float32), -4.0, 4.0)
    rough = jnp.exp(jax.random.uniform(second, (BATCH, IMG, 1), jnp.float32, math.log(0.5), math.log(2.0)))
    slope = jax.random.uniform(third, (BATCH, 1, 1), jnp.float32, -3.5, 3.5)
    place = (jnp.arange(IMG, dtype=jnp.float32) + 0.5) / IMG - 0.5
    ramp = jnp.exp(slope * place[None, :, None])
    return (base * rough * ramp).astype(jnp.bfloat16)


def draw_refresh(key, part):
    flags = jax.random.randint(jax.random.fold_in(key, 21), (BATCH,), 0, 2)
    chosen_on = jax.random.randint(jax.random.fold_in(key, 22), (), 0, BATCH)
    stride = jax.random.randint(jax.random.fold_in(key, 23), (), 0, BATCH - 1)
    chosen_off = (chosen_on + 1 + stride) % BATCH
    index = jnp.arange(BATCH, dtype=jnp.int32)
    flags = jnp.where(index == chosen_on, 1, jnp.where(index == chosen_off, 0, flags))
    return flags.astype(jnp.int32)


def touch_ends(values, key, low, top_value):
    longest = values.shape.index(max(values.shape))
    spots = []
    for shift in (0, 1):
        where = [jax.random.randint(jax.random.fold_in(key, axis), (), 0, length) for axis, length in enumerate(values.shape)]
        where[longest] = (where[longest] + shift) % values.shape[longest]
        spots.append(tuple(where))
    return values.at[spots[0]].set(low).at[spots[1]].set(top_value)


def spiked(values, rng, source, target, blocks, factor):
    owner, partner = [(jnp.arange(values.shape[position]) // (values.shape[position] // blocks)).reshape([-1 if axis == position else 1 for axis in range(values.ndim)]) for position in (source, target)]
    chosen = jax.random.permutation(rng, blocks)[partner]
    strong = (owner == chosen) | (owner == (partner + blocks // 2) % blocks)
    return jnp.where(strong, factor * values, values)


def block_scale(stream_key, extent, cuts, smallest, top_value):
    factor_of, own = 1.0, jax.random.fold_in(stream_key, 6)
    for dim, shards_of in cuts:
        draws = jnp.exp(jax.random.uniform(jax.random.fold_in(own, dim), (shards_of,), jnp.float32, smallest / len(cuts), top_value / len(cuts)))
        factor_of = factor_of * jnp.repeat(draws, extent[dim] // shards_of).reshape([-1 if axis == dim else 1 for axis in range(len(extent))])
    return factor_of


def gaussian(stream_key, extent, deviation, reach, pieces=(), kind=jnp.bfloat16):
    array = jax.random.normal(stream_key, extent, jnp.float32) * deviation
    if len(pieces) > 0:
        array = block_scale(stream_key, extent, pieces, -0.22, 0.18) * array
    return jnp.clip(array, min=-reach, max=reach).astype(kind)


def bell_draw_with(stream_key, extent, deviation, bound, shards, heavy, kind=jnp.bfloat16):
    result = deviation * jax.random.normal(stream_key, extent, jnp.float32)
    if shards:
        result = result * block_scale(stream_key, extent, shards, -0.22, 0.18)
    return jnp.clip(spiked(result, jax.random.fold_in(stream_key, 3), *heavy), -bound, bound).astype(kind)


def setup_inputs(seed: int = 0) -> dict:
    seeds = jax.random.split(jax.random.key(seed), 11)
    return {
        "img": gaussian(seeds[0], (BATCH, IMG, D), 1.0, 6.0, ((1, 16), (2, 2))),
        "txt": gaussian(seeds[1], (BATCH, TXT, D), 1.0, 6.0, ((1, 16), (2, 2))),
        "prev_mod": draw_prev_mod(jax.random.fold_in(seeds[10], 71), 0),
        "cache": gaussian(seeds[3], (BATCH, IMG, D), 1.0, 6.0, ((1, 16), (2, 2)), jnp.float32),
        "modulation": gaussian(seeds[4], (3, BATCH, D), 1.0, 4.0, ((2, 2),)),
        "w_qkv": draw_w_qkv(jax.random.fold_in(seeds[10], 71), 0),
        "qk_gain": draw_qk_gain(jax.random.fold_in(seeds[10], 71), 0),
        "output_weight": bell_draw_with(seeds[7], (HEADS * HD, D), (HEADS * HD) ** -0.5, 0.1875, ((0, 2),), (0, 1, 2, 2.0)),
        "text_len": touch_ends(jax.random.randint(seeds[8], (BATCH,), 1, TXT + 1), jax.random.fold_in(seeds[8], 1), 1, TXT).astype(jnp.int32),
        "refresh": draw_refresh(jax.random.fold_in(seeds[10], 71), 0),
    }


EPS = 0.1
NEG = -1e+30

def unit_heads(block, gain):
    shaped = block.reshape(block.shape[:-1] + (block.shape[-1] // HD, HD))
    scaled = shaped * lax.rsqrt(lax.optimization_barrier(jnp.mean(jnp.square(shaped), axis=-1, keepdims=True)) + EPS)
    return scaled.reshape(block.shape) * gain

def reference(img, txt, prev_mod, cache, modulation, w_qkv, qk_gain, output_weight, text_len, refresh):
    mods = modulation.astype(jnp.float32)
    joined = jnp.concatenate([txt, img], axis=1).astype(jnp.float32)
    center = lax.optimization_barrier(jnp.mean(joined, axis=2, keepdims=True))
    spread = lax.optimization_barrier(jnp.mean(jnp.square(joined - center), axis=2, keepdims=True))
    normed = (joined - center) * lax.rsqrt(spread + EPS)
    modded = (normed * (1.0 + mods[1][:, None, :]) + mods[0][:, None, :]).astype(jnp.bfloat16)
    image_mod = modded[:, TXT:, :].astype(jnp.float32)
    previous = prev_mod.astype(jnp.float32)
    numer = lax.optimization_barrier(jnp.sum(jnp.abs(image_mod - previous), axis=(1, 2)))
    denom = lax.optimization_barrier(jnp.sum(jnp.abs(previous), axis=(1, 2)))
    rel_l1 = numer / jnp.maximum(denom, 1.0)
    projected = jnp.einsum('btd,dkc->btkc', modded.astype(jnp.float32), w_qkv.astype(jnp.float32))
    query = unit_heads(projected[:, TXT:, 0, :], qk_gain[0]).astype(jnp.bfloat16)
    keyed = unit_heads(projected[:, :, 1, :], qk_gain[1]).astype(jnp.bfloat16)
    valued = projected[:, :, 2, :].astype(jnp.bfloat16)
    total_keys = TXT + IMG
    positions = jnp.arange(total_keys, dtype=jnp.int32)
    valid = (positions[None, :] >= TXT) | (positions[None, :] < text_len[:, None])
    query_heads = query.reshape(BATCH, IMG, HEADS, HD).transpose(2, 0, 1, 3)
    key_heads = keyed.reshape(BATCH, total_keys, HEADS, HD).transpose(2, 0, 1, 3)
    value_heads = valued.reshape(BATCH, total_keys, HEADS, HD).transpose(2, 0, 1, 3)
    score_scale = 1.0 / HD ** 0.5

    def one_head(group):
        query_slice, key_slice, value_slice = group
        logit_scores = jnp.einsum('sna,sva->snv', query_slice.astype(jnp.float32), key_slice.astype(jnp.float32)) * score_scale
        logit_scores = jnp.where(valid[:, None, :], logit_scores, NEG)
        top = lax.optimization_barrier(jnp.max(logit_scores, axis=2, keepdims=True))
        attention_weights = jnp.where(valid[:, None, :], jnp.exp(logit_scores - top), 0.0)
        total = lax.optimization_barrier(jnp.sum(attention_weights, axis=2, keepdims=True))
        summed_output = jnp.einsum('yef,yfp->yep', attention_weights.astype(jnp.bfloat16).astype(jnp.float32), value_slice.astype(jnp.float32))
        return (summed_output / total).astype(jnp.bfloat16)
    attended_values = lax.map(one_head, (query_heads, key_heads, value_heads))
    attended_values = attended_values.transpose(1, 2, 0, 3).reshape(BATCH, IMG, HEADS * HD)
    mixed_heads = jnp.einsum('pxr,ro->pxo', attended_values.astype(jnp.float32), output_weight.astype(jnp.float32))
    resid = mods[2][:, None, :] * mixed_heads
    flag = (refresh == 1)[:, None, None]
    new_cache = jnp.where(flag, resid, cache)
    out_img = img.astype(jnp.float32) + new_cache
    return (out_img, new_cache, rel_l1)
```

```python
import functools

import jax
import jax.numpy as jnp
from jax import lax
from jax.experimental import pallas as pl
from jax.experimental.pallas import tpu as pltpu
from jax.sharding import PartitionSpec as P

HD = 128
MESH = pl.DeviceIdType.MESH


EPS = 0.1
NEG = -1e30


def unit_heads(block, gain):
    shaped = block.reshape(block.shape[:-1] + (block.shape[-1] // HD, HD))
    scaled = shaped * lax.rsqrt(jnp.mean(jnp.square(shaped), axis=-1, keepdims=True) + EPS)
    return scaled.reshape(block.shape) * gain


def local(img, txt, prev_mod, cache, modulation, w_qkv, qk_gain, output_weight, text_len, refresh):
    batch, img_rows, width_loc = img.shape
    txt_rows = txt.shape[1]
    rows = txt_rows + img_rows
    joined = jnp.concatenate([txt, img], axis=1)
    local_mods = modulation.astype(jnp.float32)
    wide, wide_mod = (
        lax.all_gather(joined, "tp", axis=2, tiled=True),
        lax.all_gather(modulation, "tp", axis=2, tiled=True),
    )
    wide_mods = wide_mod.astype(jnp.float32)
    values = wide.astype(jnp.float32)
    center = jnp.mean(values, axis=2, keepdims=True)
    spread = jnp.mean(jnp.square(values - center), axis=2, keepdims=True)
    normed = (values - center) * lax.rsqrt(spread + EPS)
    modded = (normed * (1.0 + wide_mods[1][:, None, :]) + wide_mods[0][:, None, :]).astype(
        jnp.bfloat16
    )
    offset = lax.axis_index("tp") * width_loc
    own_image = lax.dynamic_slice_in_dim(modded[:, txt_rows:, :], offset, width_loc, 2)
    previous = prev_mod.astype(jnp.float32)
    gap = jnp.sum(jnp.abs(own_image.astype(jnp.float32) - previous), axis=(1, 2))
    base_sum = jnp.sum(jnp.abs(previous), axis=(1, 2))
    numer, denom = lax.psum((gap, base_sum), ("seq", "tp"))
    rel_l1 = numer / jnp.maximum(denom, 1.0)
    columns = w_qkv.shape[2]
    projected = jnp.einsum(
        "btd,dkc->btkc",
        modded,
        lax.all_gather(w_qkv, "seq", axis=0, tiled=True),
        preferred_element_type=jnp.float32,
    )
    heads = columns // HD
    query = unit_heads(projected[:, txt_rows:, 0, :], qk_gain[0]).astype(jnp.bfloat16)
    query_heads = query.reshape(batch, img_rows, heads, HD)
    keyed = unit_heads(projected[:, :, 1, :], qk_gain[1]).astype(jnp.bfloat16)
    valued = projected[:, :, 2, :].astype(jnp.bfloat16)
    paired = jnp.stack([keyed, valued], axis=2)
    score_scale = 1.0 / HD**0.5
    start_top = jnp.full((batch, heads, img_rows), NEG, jnp.float32)
    piece = lax.all_gather(paired, "seq", axis=1, tiled=True)
    top = start_top
    count = piece.shape[1]
    index = jnp.arange(count, dtype=jnp.int32)
    slot = index % rows
    text_pos = index // rows * txt_rows + slot
    valid = (slot >= txt_rows)[None, :] | (text_pos[None, :] < text_len[:, None])
    keys = piece[:, :, 0, :].reshape(batch, count, heads, HD)
    vals = piece[:, :, 1, :].reshape(batch, count, heads, HD)
    logit_scores = (
        jnp.einsum("bqhc,bkhc->bhqk", query_heads, keys, preferred_element_type=jnp.float32)
        * score_scale
    )
    logit_scores = jnp.where(valid[:, None, None, :], logit_scores, NEG)
    new_top = jnp.maximum(top, jnp.max(logit_scores, axis=3))
    attention_weights = jnp.where(
        valid[:, None, None, :], jnp.exp(logit_scores - new_top[..., None]), 0.0
    )
    total = jnp.sum(attention_weights, axis=3)
    summed_output = jnp.einsum(
        "bhqk,bkhc->bhqc",
        attention_weights.astype(jnp.bfloat16),
        vals,
        preferred_element_type=jnp.float32,
    )
    top, total, summed_output = (new_top, total, summed_output)
    attended_values = (summed_output / total[..., None]).astype(jnp.bfloat16)
    attended_values = attended_values.transpose(0, 2, 1, 3).reshape(batch, img_rows, columns)
    partial_output = jnp.einsum(
        "pxr,ro->pxo", attended_values, output_weight, preferred_element_type=jnp.float32
    )
    whole = lax.psum(partial_output.astype(jnp.bfloat16), "tp").astype(jnp.float32)
    mixed_heads = lax.dynamic_slice_in_dim(whole, lax.axis_index("tp") * width_loc, width_loc, 2)
    resid = local_mods[2][:, None, :] * mixed_heads
    flag = (refresh == 1)[:, None, None]
    new_cache = jnp.where(flag, resid, cache)
    out_img = img.astype(jnp.float32) + new_cache
    return (out_img, new_cache, rel_l1)


def head_kernel(n, dims, chunk_ref, w_ref, wout_ref, gain_ref, mask_ref, rel_ref, mixed_ref, relsum_ref,
                xbuf, wbuf, woutbuf, qbuf, kvbuf, attsrc, attcat, pbuf, rbuf, relbuf,
                local_sem, zsend, ssend, fsend, xrecv, diag_recv, wsend, wrecv, wfsend,
                kvsend, kvrecv, asend, arecv, psend, precv, rsend, rrecv):
    seq, tp, hloc, cols, half_img, groups = dims
    planes = seq // cols
    me = lax.axis_index("seq")
    t = lax.axis_index("tp")
    other = 1 - t
    z = me // cols
    col = me % cols
    xp = me + 1 - 2 * (me % 2)
    yp = me + 2 - 4 * ((me // 2) % 2)
    rows = chunk_ref.shape[1]
    width = chunk_ref.shape[2]

    barrier = pltpu.get_barrier_semaphore()

    def greet(k, carry):
        peer = lax.rem(me * tp + t + k, seq * tp)
        pl.semaphore_signal(barrier, inc=1, device_id=(peer // tp, peer % tp), device_id_type=MESH)
        return carry

    lax.fori_loop(1, seq * tp, greet, 0)

    own = pltpu.make_async_copy(chunk_ref, xbuf.at[me], local_sem.at[0])
    own.start()
    wout_copy = pltpu.make_async_copy(wout_ref, woutbuf, local_sem.at[1])
    wout_copy.start()
    pl.semaphore_wait(barrier, seq * tp - 1)

    def remote(src, dst, send, recv, device):
        return pltpu.make_async_remote_copy(
            src_ref=src, dst_ref=dst, send_sem=send, recv_sem=recv,
            device_id=device, device_id_type=MESH,
        )

    def arrived(dst, recv):
        remote(dst, dst, zsend.at[0], recv, (me, other)).wait_recv()

    pending = []

    def launch(copy):
        copy.start()
        pending.append(copy)

    for dz in range(1, planes):
        there = lax.rem(z + dz, planes) * cols + col
        launch(remote(chunk_ref, xbuf.at[me], zsend.at[dz - 1], xrecv.at[me], (there, t)))
    launch(remote(chunk_ref, xbuf.at[me], ssend.at[0, 0], xrecv.at[me], (xp, t)))
    launch(remote(chunk_ref, xbuf.at[me], ssend.at[0, 1], xrecv.at[me], (yp, t)))

    wcore = me % 2
    for k in range(hloc):
        hl = lax.rem(me + k, hloc)
        head = t * hloc + hl
        same = jnp.logical_and(head == me, wcore == t)

        @pl.when(same)
        def _():
            pltpu.make_async_copy(w_ref.at[hl], wbuf.at[me], wrecv.at[me]).start()

        @pl.when(jnp.logical_not(same))
        def _():
            remote(w_ref.at[hl], wbuf.at[me], wsend.at[k], wrecv.at[me], (head, wcore)).start()

    for dz in range(1, planes):
        src = lax.rem(z + dz, planes) * cols + col
        arrived(xbuf.at[src], xrecv.at[src])
        launch(remote(xbuf.at[src], xbuf.at[src], ssend.at[dz, 0], xrecv.at[src], (xp, t)))
        launch(remote(xbuf.at[src], xbuf.at[src], ssend.at[dz, 1], xrecv.at[src], (yp, t)))

    for dz in range(planes):
        plane = lax.rem(z + dz, planes)
        sx = plane * cols + xp % cols
        sy = plane * cols + yp % cols
        arrived(xbuf.at[sx], xrecv.at[sx])
        launch(remote(xbuf.at[sx, 0], xbuf.at[sx, 0], fsend.at[dz, 0], diag_recv.at[plane, 0], (yp, t)))
        arrived(xbuf.at[sy], xrecv.at[sy])
        launch(remote(xbuf.at[sy, 1], xbuf.at[sy, 1], fsend.at[dz, 1], diag_recv.at[plane, 1], (xp, t)))

    for k in range(seq // 2):
        slot = 2 * k + t
        arrived(wbuf.at[slot], wrecv.at[slot])
        launch(remote(wbuf.at[slot], wbuf.at[slot], wfsend.at[k], wrecv.at[slot], (me, other)))

    def send_rel(k, carry):
        peer = lax.rem(me * tp + t + k, seq * tp)
        remote(rel_ref, relbuf.at[me * tp + t], rsend.at[k], rrecv.at[me * tp + t],
               (peer // tp, peer % tp)).start()
        return carry

    lax.fori_loop(1, seq * tp, send_rel, 0)

    for k in range(seq // 2):
        slot = 2 * k + other
        arrived(wbuf.at[slot], wrecv.at[slot])
    own.wait()
    for plane in range(planes):
        sd = plane * cols + cols - 1 - col
        for half in range(2):
            arrived(xbuf.at[sd, half], diag_recv.at[plane, half])

    per = seq // groups
    gq = gain_ref[0:1, :]
    gk = gain_ref[1:2, :]

    def unit(block, gain):
        return (block * lax.rsqrt(jnp.mean(jnp.square(block), axis=1, keepdims=True) + EPS) * gain).astype(jnp.bfloat16)

    def kv_copy(g):
        part = kvbuf.at[t, pl.ds(g * per, per)]
        return remote(part, part, kvsend.at[g], kvrecv.at[g], (me, other))

    hs = seq // 2
    for g in range(groups):
        s0 = g * per
        total = jnp.dot(
            xbuf[s0:s0 + per, 0].reshape(per * rows, width),
            wbuf[:hs].reshape(width, 3 * HD), preferred_element_type=jnp.float32)
        total = total + jnp.dot(
            xbuf[s0:s0 + per, 1].reshape(per * rows, width),
            wbuf[hs:].reshape(width, 3 * HD), preferred_element_type=jnp.float32)
        q = unit(total[:, :HD], gq)
        qbuf[s0:s0 + per] = q.reshape(per, rows, HD)
        k = unit(total[:, HD:2 * HD], gk)
        v = total[:, 2 * HD:].astype(jnp.bfloat16)
        kvbuf[t, s0:s0 + per, 0] = k.reshape(per, rows, HD)
        kvbuf[t, s0:s0 + per, 1] = v.reshape(per, rows, HD)
        launch(kv_copy(g))
    for g in range(groups):
        part = kvbuf.at[other, pl.ds(g * per, per)]
        arrived(part, kvrecv.at[g])

    text = n * half_img
    for i in range(n):
        lo, hi = i * half_img, (i + 1) * half_img

        def keys(kind):
            parts = []
            for c in range(2):
                parts.append(kvbuf[c, :, kind, lo:hi, :].reshape(seq * half_img, HD))
                parts.append(kvbuf[c, :, kind, text:, :].reshape(seq * (rows - text), HD))
            return jnp.concatenate(parts, axis=0)

        q = qbuf[:, lo:hi, :].reshape(seq * half_img, HD)
        scores = lax.dot_general(q, keys(0), (((1,), (1,)), ((), ())),
                                 preferred_element_type=jnp.float32) * (1.0 / HD**0.5)
        valid = mask_ref[i:i + 1, :] > 0.0
        scores = jnp.where(valid, scores, NEG)
        top = jnp.max(scores, axis=1, keepdims=True)
        weights = jnp.where(valid, jnp.exp(scores - top), 0.0)
        total = jnp.sum(weights, axis=1, keepdims=True)
        summed = jnp.dot(weights.astype(jnp.bfloat16), keys(1), preferred_element_type=jnp.float32)
        attsrc[:, lo:hi, :] = (summed / total).astype(jnp.bfloat16).reshape(seq, half_img, HD)

    home = me // hloc
    hl = me % hloc
    mine = attcat.at[pl.ds(pl.multiple_of(t * text, half_img), text), pl.ds(pl.multiple_of(hl * HD, HD), HD)]
    for k in range(seq):
        s = lax.rem(me + k, seq)
        if k == 0:
            same = home == t

            @pl.when(same)
            def _():
                pltpu.make_async_copy(attsrc.at[s], mine, arecv.at[hl * 2 + t]).start()

            @pl.when(jnp.logical_not(same))
            def _():
                remote(attsrc.at[s], mine, asend.at[k], arecv.at[hl * 2 + t], (s, home)).start()
        else:
            launch(remote(attsrc.at[s], mine, asend.at[k], arecv.at[hl * 2 + t], (s, home)))
    wout_copy.wait()
    for h in range(hloc):
        for c in range(2):
            arrived(attcat.at[pl.ds(c * text, text), pl.ds(h * HD, HD)], arecv.at[h * 2 + c])

    out_width = mixed_ref.shape[1]
    acts = attcat[...]
    theirs = jnp.dot(acts, woutbuf[:, pl.ds(pl.multiple_of(other * out_width, 128), out_width)],
                     preferred_element_type=jnp.float32)
    pbuf[...] = theirs.astype(jnp.bfloat16)
    give = remote(pbuf, rbuf, psend.at[0], precv.at[0], (me, other))
    launch(give)
    ours = jnp.dot(acts, woutbuf[:, pl.ds(pl.multiple_of(t * out_width, 128), out_width)],
                   preferred_element_type=jnp.float32)

    relbuf[me * tp + t] = rel_ref[...]

    def wait_rel(k, carry):
        peer = lax.rem(me * tp + t + k, seq * tp)
        arrived(relbuf.at[peer], rrecv.at[peer])
        remote(rel_ref, relbuf.at[me * tp + t], rsend.at[k], rrecv.at[me * tp + t],
               (peer // tp, peer % tp)).wait_send()
        return carry

    lax.fori_loop(1, seq * tp, wait_rel, 0)
    relsum_ref[...] = jnp.sum(relbuf[...], axis=0)

    give.wait_recv()
    mixed_ref[...] = ours + rbuf[...].astype(jnp.float32)

    for copy in pending:
        copy.wait_send()
    for k in range(hloc):
        hl_k = lax.rem(me + k, hloc)
        same_k = jnp.logical_and(t * hloc + hl_k == me, wcore == t)

        @pl.when(jnp.logical_not(same_k))
        def _():
            remote(w_ref.at[hl_k], wbuf.at[me], wsend.at[k], wrecv.at[me], (t * hloc + hl_k, wcore)).wait_send()

    @pl.when(home != t)
    def _():
        remote(attsrc.at[me], mine, asend.at[0], arecv.at[hl * 2 + t], (me, home)).wait_send()


def head_call(n, seq, tp, half_img, cid, chunk, w_heads, wout, gain, mask, rel):
    cols = 4
    planes = seq // cols
    groups = 4
    hloc, depth, three = w_heads.shape
    rows, width = chunk.shape[1:]
    dims = (seq, tp, hloc, cols, half_img, groups)
    out_rows, out_width = n * half_img * tp, wout.shape[1] // tp
    dma = pltpu.SemaphoreType.DMA
    bf16 = jnp.bfloat16
    vmem = pl.BlockSpec(memory_space=pltpu.VMEM)
    hbm = pl.BlockSpec(memory_space=pl.ANY)
    return pl.pallas_call(
        functools.partial(head_kernel, n, dims),
        out_shape=(
            jax.ShapeDtypeStruct((out_rows, out_width), jnp.float32),
            jax.ShapeDtypeStruct(rel.shape, jnp.float32),
        ),
        in_specs=[vmem, hbm, hbm, vmem, vmem, vmem],
        out_specs=(vmem, vmem),
        scratch_shapes=[
            pltpu.VMEM((seq, 2, rows, width), bf16),
            pltpu.VMEM((seq, depth, three), bf16),
            pltpu.VMEM(wout.shape, bf16),
            pltpu.VMEM((seq, rows, HD), bf16),
            pltpu.VMEM((tp, seq, 2, rows, HD), bf16),
            pltpu.VMEM((seq, n * half_img, HD), bf16),
            pltpu.VMEM((out_rows, hloc * HD), bf16),
            pltpu.VMEM((out_rows, out_width), bf16),
            pltpu.VMEM((out_rows, out_width), bf16),
            pltpu.VMEM((seq * tp,) + rel.shape, jnp.float32),
            dma((2,)),
            dma((planes,)),
            dma((planes, 2)),
            dma((planes, 2)),
            dma((seq,)),
            dma((planes, 2)),
            dma((hloc,)),
            dma((seq,)),
            dma((seq // 2,)),
            dma((groups,)),
            dma((groups,)),
            dma((seq,)),
            dma((seq,)),
            dma((1,)),
            dma((1,)),
            dma((seq * tp,)),
            dma((seq * tp,)),
        ],
        compiler_params=pltpu.CompilerParams(
            collective_id=cid, has_side_effects=True, vmem_limit_bytes=58 * 1024 * 1024
        ),
    )(chunk, w_heads, wout, gain, mask, rel)


def by_heads(seq, tp, img, txt, prev_mod, cache, modulation, w_qkv, qk_gain, output_weight, text_len, refresh):
    batch, img_rows, width_loc = img.shape
    txt_rows = txt.shape[1]
    me, t = lax.axis_index("seq"), lax.axis_index("tp")
    hloc = w_qkv.shape[2] // HD
    joined = jnp.concatenate([txt, img], axis=1)
    local_mods = modulation.astype(jnp.float32)
    wide = lax.all_gather(joined, "tp", axis=2, tiled=True)
    n_mod = modulation.shape[0] * batch * width_loc
    small = jnp.concatenate([local_mods.reshape(n_mod), qk_gain.reshape(-1)])
    small = lax.all_gather(small, "tp", axis=0)
    wide_mods = small[:, :n_mod].reshape(tp, 3, batch, width_loc).transpose(1, 2, 0, 3).reshape(3, batch, tp * width_loc)
    gains = small[:, n_mod:].reshape(tp, 2, hloc, HD).transpose(1, 0, 2, 3).reshape(2, tp * hloc, HD)
    gain = lax.dynamic_index_in_dim(gains, me, 1, keepdims=False)
    values = wide.astype(jnp.float32)
    center = jnp.mean(values, axis=2, keepdims=True)
    spread = jnp.mean(jnp.square(values - center), axis=2, keepdims=True)
    scale = lax.rsqrt(spread + EPS)

    def modulate(block, mid, inv, mods):
        return ((block - mid) * inv * (1.0 + mods[1][:, None, :]) + mods[0][:, None, :]).astype(jnp.bfloat16)

    own_image = modulate(img.astype(jnp.float32), center[:, txt_rows:], scale[:, txt_rows:], local_mods)
    previous = prev_mod.astype(jnp.float32)
    gap = jnp.sum(jnp.abs(own_image.astype(jnp.float32) - previous), axis=(1, 2))
    base_sum = jnp.sum(jnp.abs(previous), axis=(1, 2))
    rel = jnp.broadcast_to(jnp.stack([gap, base_sum]).reshape(2 * batch, 1), (2 * batch, 128))

    on = refresh == 1
    rank = jnp.cumsum(on.astype(jnp.int32)) - on.astype(jnp.int32)
    w_heads = w_qkv.reshape(w_qkv.shape[0], 3, hloc, HD).transpose(2, 0, 1, 3).reshape(hloc, w_qkv.shape[0], 3 * HD)
    half_img, half_txt = img_rows // tp, txt_rows // tp

    def run(n, cid):
        slots = jnp.arange(n, dtype=jnp.int32)
        hit = on[None, :] & (rank[None, :] == slots[:, None])
        sel = jnp.sum(jnp.where(hit, jnp.arange(batch, dtype=jnp.int32)[None, :], 0), axis=1)
        pad = -(-n * half_txt // 16) * 16
        rows_i = lax.dynamic_slice_in_dim(values, txt_rows + t * half_img, half_img, 1)
        rows_t = lax.dynamic_slice_in_dim(values, t * half_txt, half_txt, 1)
        mid_i = lax.dynamic_slice_in_dim(center, txt_rows + t * half_img, half_img, 1)
        mid_t = lax.dynamic_slice_in_dim(center, t * half_txt, half_txt, 1)
        inv_i = lax.dynamic_slice_in_dim(scale, txt_rows + t * half_img, half_img, 1)
        inv_t = lax.dynamic_slice_in_dim(scale, t * half_txt, half_txt, 1)
        mod_i = modulate(rows_i, mid_i, inv_i, wide_mods)
        mod_t = modulate(rows_t, mid_t, inv_t, wide_mods)
        pick = lambda a: jnp.concatenate([lax.dynamic_slice_in_dim(a, sel[i], 1, 0) for i in range(n)], axis=0)
        mod_i = pick(mod_i).reshape(n * half_img, -1)
        mod_t = pick(mod_t).reshape(n * half_txt, -1)
        mod_t = jnp.pad(mod_t, ((0, pad - n * half_txt), (0, 0)))
        chunk = jnp.concatenate([mod_i, mod_t], axis=0)
        chunk = jnp.stack([chunk[:, :width_loc], chunk[:, width_loc:]])
        r = jnp.arange(pad, dtype=jnp.int32)
        pos = (jnp.arange(seq, dtype=jnp.int32)[None, :, None] * txt_rows
               + jnp.arange(tp, dtype=jnp.int32)[:, None, None] * half_txt + (r % half_txt)[None, None, :])
        lens = jnp.stack([lax.dynamic_index_in_dim(text_len, sel[i], 0, keepdims=False) for i in range(n)])
        ok_t = ((r // half_txt)[None, None, None, :] == slots[:, None, None, None]) & (pos[None] < lens[:, None, None, None])
        ok_t = ok_t.reshape(n, tp, seq * pad)
        ok_i = jnp.ones((n, tp, seq * half_img), bool)
        mask = jnp.concatenate([ok_i, ok_t], axis=2).reshape(n, -1).astype(jnp.float32)
        mixed, sums = head_call(n, seq, tp, half_img, cid, chunk, w_heads, output_weight, gain, mask, rel)
        mixed = mixed.reshape(tp, n, half_img, width_loc).transpose(1, 0, 2, 3).reshape(n, img_rows, width_loc)
        back = jnp.minimum(rank, n - 1)
        whole = jnp.concatenate([lax.dynamic_slice_in_dim(mixed, back[b], 1, 0) for b in range(batch)], axis=0)
        resid = local_mods[2][:, None, :] * whole
        new_cache = jnp.where(on[:, None, None], resid, cache)
        out_img = img.astype(jnp.float32) + new_cache
        numer, denom = sums[:batch, 0], sums[batch:, 0]
        return out_img, new_cache, numer / jnp.maximum(denom, 1.0)

    return run(batch - 1, 0)


def solution(mesh):
    seq, tp = mesh.shape["seq"], mesh.shape["tp"]

    def step(*args):
        img, txt, w_qkv = args[0], args[1], args[5]
        hloc = w_qkv.shape[2] // HD
        fits = (
            tp == 2 and seq % 8 == 0 and hloc * tp == seq and img.shape[0] == 4
            and img.shape[1] % 32 == 0 and txt.shape[1] % 2 == 0
        )
        if fits:
            return by_heads(seq, tp, *args)
        return local(*args)

    return jax.shard_map(
        step,
        mesh=mesh,
        in_specs=(
            P(None, "seq", "tp"),
            P(None, "seq", "tp"),
            P(None, "seq", "tp"),
            P(None, "seq", "tp"),
            P(None, None, "tp"),
            P("seq", None, "tp"),
            P(None, "tp"),
            P("tp", None),
            P(),
            P(),
        ),
        out_specs=(P(None, "seq", "tp"), P(None, "seq", "tp"), P()),
        check_vma=False,
    )
```

```python
import functools

import jax
import jax.numpy as jnp
from jax import lax
from jax.experimental import pallas as pl
from jax.experimental.pallas import tpu as pltpu
from jax.sharding import PartitionSpec as P

HD = 128
MESH = pl.DeviceIdType.MESH


EPS = 0.1
NEG = -1e30


def unit_heads(block, gain):
    shaped = block.reshape(block.shape[:-1] + (block.shape[-1] // HD, HD))
    scaled = shaped * lax.rsqrt(jnp.mean(jnp.square(shaped), axis=-1, keepdims=True) + EPS)
    return scaled.reshape(block.shape) * gain


def local(img, txt, prev_mod, cache, modulation, w_qkv, qk_gain, output_weight, text_len, refresh):
    batch, img_rows, width_loc = img.shape
    txt_rows = txt.shape[1]
    rows = txt_rows + img_rows
    joined = jnp.concatenate([txt, img], axis=1)
    local_mods = modulation.astype(jnp.float32)
    wide, wide_mod = (
        lax.all_gather(joined, "tp", axis=2, tiled=True),
        lax.all_gather(modulation, "tp", axis=2, tiled=True),
    )
    wide_mods = wide_mod.astype(jnp.float32)
    values = wide.astype(jnp.float32)
    center = jnp.mean(values, axis=2, keepdims=True)
    spread = jnp.mean(jnp.square(values - center), axis=2, keepdims=True)
    normed = (values - center) * lax.rsqrt(spread + EPS)
    modded = (normed * (1.0 + wide_mods[1][:, None, :]) + wide_mods[0][:, None, :]).astype(
        jnp.bfloat16
    )
    offset = lax.axis_index("tp") * width_loc
    own_image = lax.dynamic_slice_in_dim(modded[:, txt_rows:, :], offset, width_loc, 2)
    previous = prev_mod.astype(jnp.float32)
    gap = jnp.sum(jnp.abs(own_image.astype(jnp.float32) - previous), axis=(1, 2))
    base_sum = jnp.sum(jnp.abs(previous), axis=(1, 2))
    numer, denom = lax.psum((gap, base_sum), ("seq", "tp"))
    rel_l1 = numer / jnp.maximum(denom, 1.0)
    columns = w_qkv.shape[2]
    projected = jnp.einsum(
        "btd,dkc->btkc",
        modded,
        lax.all_gather(w_qkv, "seq", axis=0, tiled=True),
        preferred_element_type=jnp.float32,
    )
    heads = columns // HD
    query = unit_heads(projected[:, txt_rows:, 0, :], qk_gain[0]).astype(jnp.bfloat16)
    query_heads = query.reshape(batch, img_rows, heads, HD)
    keyed = unit_heads(projected[:, :, 1, :], qk_gain[1]).astype(jnp.bfloat16)
    valued = projected[:, :, 2, :].astype(jnp.bfloat16)
    paired = jnp.stack([keyed, valued], axis=2)
    score_scale = 1.0 / HD**0.5
    start_top = jnp.full((batch, heads, img_rows), NEG, jnp.float32)
    piece = lax.all_gather(paired, "seq", axis=1, tiled=True)
    top = start_top
    count = piece.shape[1]
    index = jnp.arange(count, dtype=jnp.int32)
    slot = index % rows
    text_pos = index // rows * txt_rows + slot
    valid = (slot >= txt_rows)[None, :] | (text_pos[None, :] < text_len[:, None])
    keys = piece[:, :, 0, :].reshape(batch, count, heads, HD)
    vals = piece[:, :, 1, :].reshape(batch, count, heads, HD)
    logit_scores = (
        jnp.einsum("bqhc,bkhc->bhqk", query_heads, keys, preferred_element_type=jnp.float32)
        * score_scale
    )
    logit_scores = jnp.where(valid[:, None, None, :], logit_scores, NEG)
    new_top = jnp.maximum(top, jnp.max(logit_scores, axis=3))
    attention_weights = jnp.where(
        valid[:, None, None, :], jnp.exp(logit_scores - new_top[..., None]), 0.0
    )
    total = jnp.sum(attention_weights, axis=3)
    summed_output = jnp.einsum(
        "bhqk,bkhc->bhqc",
        attention_weights.astype(jnp.bfloat16),
        vals,
        preferred_element_type=jnp.float32,
    )
    top, total, summed_output = (new_top, total, summed_output)
    attended_values = (summed_output / total[..., None]).astype(jnp.bfloat16)
    attended_values = attended_values.transpose(0, 2, 1, 3).reshape(batch, img_rows, columns)
    partial_output = jnp.einsum(
        "pxr,ro->pxo", attended_values, output_weight, preferred_element_type=jnp.float32
    )
    whole = lax.psum(partial_output.astype(jnp.bfloat16), "tp").astype(jnp.float32)
    mixed_heads = lax.dynamic_slice_in_dim(whole, lax.axis_index("tp") * width_loc, width_loc, 2)
    resid = local_mods[2][:, None, :] * mixed_heads
    flag = (refresh == 1)[:, None, None]
    new_cache = jnp.where(flag, resid, cache)
    out_img = img.astype(jnp.float32) + new_cache
    return (out_img, new_cache, rel_l1)


def head_kernel(n, dims, chunk_ref, w_ref, wout_ref, gain_ref, mask_ref, rel_ref, mixed_ref, relsum_ref,
                xbuf, wbuf, woutbuf, qbuf, kvbuf, attsrc, attcat, pbuf, rbuf, relbuf,
                local_sem, zsend, ssend, fsend, xrecv, diag_recv, wsend, wrecv, wfsend,
                kvsend, kvrecv, asend, arecv, psend, precv, rsend, rrecv):
    seq, tp, hloc, cols, half_img, groups = dims
    planes = seq // cols
    me = lax.axis_index("seq")
    t = lax.axis_index("tp")
    other = 1 - t
    z = me // cols
    col = me % cols
    xp = me + 1 - 2 * (me % 2)
    yp = me + 2 - 4 * ((me // 2) % 2)
    rows = chunk_ref.shape[1]
    width = chunk_ref.shape[2]

    barrier = pltpu.get_barrier_semaphore()

    def greet(k, carry):
        peer = lax.rem(me * tp + t + k, seq * tp)
        pl.semaphore_signal(barrier, inc=1, device_id=(peer // tp, peer % tp), device_id_type=MESH)
        return carry

    lax.fori_loop(1, seq * tp, greet, 0)

    own = pltpu.make_async_copy(chunk_ref, xbuf.at[me], local_sem.at[0])
    own.start()
    wout_copy = pltpu.make_async_copy(wout_ref, woutbuf, local_sem.at[1])
    wout_copy.start()
    pl.semaphore_wait(barrier, seq * tp - 1)

    def remote(src, dst, send, recv, device):
        return pltpu.make_async_remote_copy(
            src_ref=src, dst_ref=dst, send_sem=send, recv_sem=recv,
            device_id=device, device_id_type=MESH,
        )

    def arrived(dst, recv):
        remote(dst, dst, zsend.at[0], recv, (me, other)).wait_recv()

    pending = []

    def launch(copy):
        copy.start()
        pending.append(copy)

    for dz in range(1, planes):
        there = lax.rem(z + dz, planes) * cols + col
        launch(remote(chunk_ref, xbuf.at[me], zsend.at[dz - 1], xrecv.at[me], (there, t)))
    launch(remote(chunk_ref, xbuf.at[me], ssend.at[0, 0], xrecv.at[me], (xp, t)))
    launch(remote(chunk_ref, xbuf.at[me], ssend.at[0, 1], xrecv.at[me], (yp, t)))

    wcore = me % 2
    for k in range(hloc):
        hl = lax.rem(me + k, hloc)
        head = t * hloc + hl
        same = jnp.logical_and(head == me, wcore == t)

        @pl.when(same)
        def _():
            pltpu.make_async_copy(w_ref.at[hl], wbuf.at[me], wrecv.at[me]).start()

        @pl.when(jnp.logical_not(same))
        def _():
            remote(w_ref.at[hl], wbuf.at[me], wsend.at[k], wrecv.at[me], (head, wcore)).start()

    for dz in range(1, planes):
        src = lax.rem(z + dz, planes) * cols + col
        arrived(xbuf.at[src], xrecv.at[src])
        launch(remote(xbuf.at[src], xbuf.at[src], ssend.at[dz, 0], xrecv.at[src], (xp, t)))
        launch(remote(xbuf.at[src], xbuf.at[src], ssend.at[dz, 1], xrecv.at[src], (yp, t)))

    for dz in range(planes):
        plane = lax.rem(z + dz, planes)
        sx = plane * cols + xp % cols
        sy = plane * cols + yp % cols
        arrived(xbuf.at[sx], xrecv.at[sx])
        launch(remote(xbuf.at[sx, 0], xbuf.at[sx, 0], fsend.at[dz, 0], diag_recv.at[plane, 0], (yp, t)))
        arrived(xbuf.at[sy], xrecv.at[sy])
        launch(remote(xbuf.at[sy, 1], xbuf.at[sy, 1], fsend.at[dz, 1], diag_recv.at[plane, 1], (xp, t)))

    for k in range(seq // 2):
        slot = 2 * k + t
        arrived(wbuf.at[slot], wrecv.at[slot])
        launch(remote(wbuf.at[slot], wbuf.at[slot], wfsend.at[k], wrecv.at[slot], (me, other)))

    def send_rel(k, carry):
        peer = lax.rem(me * tp + t + k, seq * tp)
        remote(rel_ref, relbuf.at[me * tp + t], rsend.at[k], rrecv.at[me * tp + t],
               (peer // tp, peer % tp)).start()
        return carry

    lax.fori_loop(1, seq * tp, send_rel, 0)

    for k in range(seq // 2):
        slot = 2 * k + other
        arrived(wbuf.at[slot], wrecv.at[slot])
    own.wait()
    for plane in range(planes):
        sd = plane * cols + cols - 1 - col
        for half in range(2):
            arrived(xbuf.at[sd, half], diag_recv.at[plane, half])

    per = seq // groups
    gq = gain_ref[0:1, :]
    gk = gain_ref[1:2, :]

    def unit(block, gain):
        return (block * lax.rsqrt(jnp.mean(jnp.square(block), axis=1, keepdims=True) + EPS) * gain).astype(jnp.bfloat16)

    def kv_copy(g):
        part = kvbuf.at[t, pl.ds(g * per, per)]
        return remote(part, part, kvsend.at[g], kvrecv.at[g], (me, other))

    hs = seq // 2
    for g in range(groups):
        s0 = g * per
        total = jnp.dot(
            xbuf[s0:s0 + per, 0].reshape(per * rows, width),
            wbuf[:hs].reshape(width, 3 * HD), preferred_element_type=jnp.float32)
        total = total + jnp.dot(
            xbuf[s0:s0 + per, 1].reshape(per * rows, width),
            wbuf[hs:].reshape(width, 3 * HD), preferred_element_type=jnp.float32)
        q = unit(total[:, :HD], gq)
        qbuf[s0:s0 + per] = q.reshape(per, rows, HD)
        k = unit(total[:, HD:2 * HD], gk)
        v = total[:, 2 * HD:].astype(jnp.bfloat16)
        kvbuf[t, s0:s0 + per, 0] = k.reshape(per, rows, HD)
        kvbuf[t, s0:s0 + per, 1] = v.reshape(per, rows, HD)
        launch(kv_copy(g))
    for g in range(groups):
        part = kvbuf.at[other, pl.ds(g * per, per)]
        arrived(part, kvrecv.at[g])

    text = n * half_img
    for i in range(n):
        lo, hi = i * half_img, (i + 1) * half_img

        def keys(kind):
            parts = []
            for c in range(2):
                parts.append(kvbuf[c, :, kind, lo:hi, :].reshape(seq * half_img, HD))
                parts.append(kvbuf[c, :, kind, text:, :].reshape(seq * (rows - text), HD))
            return jnp.concatenate(parts, axis=0)

        q = qbuf[:, lo:hi, :].reshape(seq * half_img, HD)
        scores = lax.dot_general(q, keys(0), (((1,), (1,)), ((), ())),
                                 preferred_element_type=jnp.float32) * (1.0 / HD**0.5)
        valid = mask_ref[i:i + 1, :] > 0.0
        scores = jnp.where(valid, scores, NEG)
        top = jnp.max(scores, axis=1, keepdims=True)
        weights = jnp.where(valid, jnp.exp(scores - top), 0.0)
        total = jnp.sum(weights, axis=1, keepdims=True)
        summed = jnp.dot(weights.astype(jnp.bfloat16), keys(1), preferred_element_type=jnp.float32)
        attsrc[:, lo:hi, :] = (summed / total).astype(jnp.bfloat16).reshape(seq, half_img, HD)

    home = me // hloc
    hl = me % hloc
    mine = attcat.at[pl.ds(pl.multiple_of(t * text, half_img), text), pl.ds(pl.multiple_of(hl * HD, HD), HD)]
    for k in range(seq):
        s = lax.rem(me + k, seq)
        if k == 0:
            same = home == t

            @pl.when(same)
            def _():
                pltpu.make_async_copy(attsrc.at[s], mine, arecv.at[hl * 2 + t]).start()

            @pl.when(jnp.logical_not(same))
            def _():
                remote(attsrc.at[s], mine, asend.at[k], arecv.at[hl * 2 + t], (s, home)).start()
        else:
            launch(remote(attsrc.at[s], mine, asend.at[k], arecv.at[hl * 2 + t], (s, home)))
    wout_copy.wait()
    for h in range(hloc):
        for c in range(2):
            arrived(attcat.at[pl.ds(c * text, text), pl.ds(h * HD, HD)], arecv.at[h * 2 + c])

    out_width = mixed_ref.shape[1]
    acts = attcat[...]
    theirs = jnp.dot(acts, woutbuf[:, pl.ds(pl.multiple_of(other * out_width, 128), out_width)],
                     preferred_element_type=jnp.float32)
    pbuf[...] = theirs.astype(jnp.bfloat16)
    give = remote(pbuf, rbuf, psend.at[0], precv.at[0], (me, other))
    launch(give)
    ours = jnp.dot(acts, woutbuf[:, pl.ds(pl.multiple_of(t * out_width, 128), out_width)],
                   preferred_element_type=jnp.float32)

    relbuf[me * tp + t] = rel_ref[...]

    def wait_rel(k, carry):
        peer = lax.rem(me * tp + t + k, seq * tp)
        arrived(relbuf.at[peer], rrecv.at[peer])
        remote(rel_ref, relbuf.at[me * tp + t], rsend.at[k], rrecv.at[me * tp + t],
               (peer // tp, peer % tp)).wait_send()
        return carry

    lax.fori_loop(1, seq * tp, wait_rel, 0)
    relsum_ref[...] = jnp.sum(relbuf[...], axis=0)

    give.wait_recv()
    mixed_ref[...] = ours + rbuf[...].astype(jnp.float32)

    for copy in pending:
        copy.wait_send()
    for k in range(hloc):
        hl_k = lax.rem(me + k, hloc)
        same_k = jnp.logical_and(t * hloc + hl_k == me, wcore == t)

        @pl.when(jnp.logical_not(same_k))
        def _():
            remote(w_ref.at[hl_k], wbuf.at[me], wsend.at[k], wrecv.at[me], (t * hloc + hl_k, wcore)).wait_send()

    @pl.when(home != t)
    def _():
        remote(attsrc.at[me], mine, asend.at[0], arecv.at[hl * 2 + t], (me, home)).wait_send()


def head_call(n, seq, tp, half_img, cid, chunk, w_heads, wout, gain, mask, rel):
    cols = 4
    planes = seq // cols
    groups = 4
    hloc, depth, three = w_heads.shape
    rows, width = chunk.shape[1:]
    dims = (seq, tp, hloc, cols, half_img, groups)
    out_rows, out_width = n * half_img * tp, wout.shape[1] // tp
    dma = pltpu.SemaphoreType.DMA
    bf16 = jnp.bfloat16
    vmem = pl.BlockSpec(memory_space=pltpu.VMEM)
    hbm = pl.BlockSpec(memory_space=pl.ANY)
    return pl.pallas_call(
        functools.partial(head_kernel, n, dims),
        out_shape=(
            jax.ShapeDtypeStruct((out_rows, out_width), jnp.float32),
            jax.ShapeDtypeStruct(rel.shape, jnp.float32),
        ),
        in_specs=[vmem, hbm, hbm, vmem, vmem, vmem],
        out_specs=(vmem, vmem),
        scratch_shapes=[
            pltpu.VMEM((seq, 2, rows, width), bf16),
            pltpu.VMEM((seq, depth, three), bf16),
            pltpu.VMEM(wout.shape, bf16),
            pltpu.VMEM((seq, rows, HD), bf16),
            pltpu.VMEM((tp, seq, 2, rows, HD), bf16),
            pltpu.VMEM((seq, n * half_img, HD), bf16),
            pltpu.VMEM((out_rows, hloc * HD), bf16),
            pltpu.VMEM((out_rows, out_width), bf16),
            pltpu.VMEM((out_rows, out_width), bf16),
            pltpu.VMEM((seq * tp,) + rel.shape, jnp.float32),
            dma((2,)),
            dma((planes,)),
            dma((planes, 2)),
            dma((planes, 2)),
            dma((seq,)),
            dma((planes, 2)),
            dma((hloc,)),
            dma((seq,)),
            dma((seq // 2,)),
            dma((groups,)),
            dma((groups,)),
            dma((seq,)),
            dma((seq,)),
            dma((1,)),
            dma((1,)),
            dma((seq * tp,)),
            dma((seq * tp,)),
        ],
        compiler_params=pltpu.CompilerParams(
            collective_id=cid, has_side_effects=True, vmem_limit_bytes=58 * 1024 * 1024
        ),
    )(chunk, w_heads, wout, gain, mask, rel)


def by_heads(seq, tp, img, txt, prev_mod, cache, modulation, w_qkv, qk_gain, output_weight, text_len, refresh):
    batch, img_rows, width_loc = img.shape
    txt_rows = txt.shape[1]
    me, t = lax.axis_index("seq"), lax.axis_index("tp")
    hloc = w_qkv.shape[2] // HD
    joined = jnp.concatenate([txt, img], axis=1)
    local_mods = modulation.astype(jnp.float32)
    wide = lax.all_gather(joined, "tp", axis=2, tiled=True)
    n_mod = modulation.shape[0] * batch * width_loc
    small = jnp.concatenate([local_mods.reshape(n_mod), qk_gain.reshape(-1)])
    small = lax.all_gather(small, "tp", axis=0)
    wide_mods = small[:, :n_mod].reshape(tp, 3, batch, width_loc).transpose(1, 2, 0, 3).reshape(3, batch, tp * width_loc)
    gains = small[:, n_mod:].reshape(tp, 2, hloc, HD).transpose(1, 0, 2, 3).reshape(2, tp * hloc, HD)
    gain = lax.dynamic_index_in_dim(gains, me, 1, keepdims=False)
    values = wide.astype(jnp.float32)
    center = jnp.mean(values, axis=2, keepdims=True)
    spread = jnp.mean(jnp.square(values - center), axis=2, keepdims=True)
    scale = lax.rsqrt(spread + EPS)

    def modulate(block, mid, inv, mods):
        return ((block - mid) * inv * (1.0 + mods[1][:, None, :]) + mods[0][:, None, :]).astype(jnp.bfloat16)

    own_image = modulate(img.astype(jnp.float32), center[:, txt_rows:], scale[:, txt_rows:], local_mods)
    previous = prev_mod.astype(jnp.float32)
    gap = jnp.sum(jnp.abs(own_image.astype(jnp.float32) - previous), axis=(1, 2))
    base_sum = jnp.sum(jnp.abs(previous), axis=(1, 2))
    rel = jnp.broadcast_to(jnp.stack([gap, base_sum]).reshape(2 * batch, 1), (2 * batch, 128))

    on = refresh == 1
    rank = jnp.cumsum(on.astype(jnp.int32)) - on.astype(jnp.int32)
    w_heads = w_qkv.reshape(w_qkv.shape[0], 3, hloc, HD).transpose(2, 0, 1, 3).reshape(hloc, w_qkv.shape[0], 3 * HD)
    half_img, half_txt = img_rows // tp, txt_rows // tp

    def run(n, cid):
        slots = jnp.arange(n, dtype=jnp.int32)
        hit = on[None, :] & (rank[None, :] == slots[:, None])
        pad = -(-n * half_txt // 8) * 8
        rows_i = lax.dynamic_slice_in_dim(values, txt_rows + t * half_img, half_img, 1)
        rows_t = lax.dynamic_slice_in_dim(values, t * half_txt, half_txt, 1)
        mid_i = lax.dynamic_slice_in_dim(center, txt_rows + t * half_img, half_img, 1)
        mid_t = lax.dynamic_slice_in_dim(center, t * half_txt, half_txt, 1)
        inv_i = lax.dynamic_slice_in_dim(scale, txt_rows + t * half_img, half_img, 1)
        inv_t = lax.dynamic_slice_in_dim(scale, t * half_txt, half_txt, 1)
        mod_i = modulate(rows_i, mid_i, inv_i, wide_mods)
        mod_t = modulate(rows_t, mid_t, inv_t, wide_mods)

        def pick(a):
            taken = a[batch - 1][None]
            for b in range(batch - 1):
                taken = jnp.where(hit[:, b, None, None], a[b][None], taken)
            return taken

        mod_i = pick(mod_i).reshape(n * half_img, -1)
        mod_t = pick(mod_t).reshape(n * half_txt, -1)
        mod_t = jnp.pad(mod_t, ((0, pad - n * half_txt), (0, 0)))
        chunk = jnp.concatenate([mod_i, mod_t], axis=0)
        chunk = jnp.stack([chunk[:, :width_loc], chunk[:, width_loc:]])
        r = jnp.arange(pad, dtype=jnp.int32)
        pos = (jnp.arange(seq, dtype=jnp.int32)[None, :, None] * txt_rows
               + jnp.arange(tp, dtype=jnp.int32)[:, None, None] * half_txt + (r % half_txt)[None, None, :])
        lens = jnp.sum(jnp.where(hit, text_len[None, :], 0), axis=1)
        ok_t = ((r // half_txt)[None, None, None, :] == slots[:, None, None, None]) & (pos[None] < lens[:, None, None, None])
        ok_t = ok_t.reshape(n, tp, seq * pad)
        ok_i = jnp.ones((n, tp, seq * half_img), bool)
        mask = jnp.concatenate([ok_i, ok_t], axis=2).reshape(n, -1).astype(jnp.float32)
        mixed, sums = head_call(n, seq, tp, half_img, cid, chunk, w_heads, output_weight, gain, mask, rel)
        mixed = mixed.reshape(tp, n, half_img, width_loc).transpose(1, 0, 2, 3).reshape(n, img_rows, width_loc)
        whole = mixed[n - 1][None]
        for k in range(n - 1):
            whole = jnp.where((rank == k)[:, None, None], mixed[k][None], whole)
        return jnp.broadcast_to(whole, img.shape), sums

    level = jnp.clip(jnp.sum(on.astype(jnp.int32)) - 1, 0, batch - 2)
    whole, sums = lax.switch(level, [functools.partial(run, k + 1, k) for k in range(batch - 1)])
    resid = local_mods[2][:, None, :] * whole
    new_cache = jnp.where(on[:, None, None], resid, cache)
    out_img = img.astype(jnp.float32) + new_cache
    numer, denom = sums[:batch, 0], sums[batch:, 0]
    return out_img, new_cache, numer / jnp.maximum(denom, 1.0)


def solution(mesh):
    seq, tp = mesh.shape["seq"], mesh.shape["tp"]

    def step(*args):
        img, txt, w_qkv = args[0], args[1], args[5]
        hloc = w_qkv.shape[2] // HD
        fits = (
            tp == 2 and seq % 8 == 0 and hloc * tp == seq and img.shape[0] == 4
            and img.shape[1] % 32 == 0 and txt.shape[1] % 2 == 0
        )
        if fits:
            return by_heads(seq, tp, *args)
        return local(*args)

    return jax.shard_map(
        step,
        mesh=mesh,
        in_specs=(
            P(None, "seq", "tp"),
            P(None, "seq", "tp"),
            P(None, "seq", "tp"),
            P(None, "seq", "tp"),
            P(None, None, "tp"),
            P("seq", None, "tp"),
            P(None, "tp"),
            P("tp", None),
            P(),
            P(),
        ),
        out_specs=(P(None, "seq", "tp"), P(None, "seq", "tp"), P()),
        check_vma=False,
    )
```

```python
import functools

import jax
import jax.numpy as jnp
from jax import lax
from jax.experimental import pallas as pl
from jax.experimental.pallas import tpu as pltpu
from jax.sharding import PartitionSpec as P

HD = 128
MESH = pl.DeviceIdType.MESH


EPS = 0.1
NEG = -1e30


def unit_heads(block, gain):
    shaped = block.reshape(block.shape[:-1] + (block.shape[-1] // HD, HD))
    scaled = shaped * lax.rsqrt(jnp.mean(jnp.square(shaped), axis=-1, keepdims=True) + EPS)
    return scaled.reshape(block.shape) * gain


def local(img, txt, prev_mod, cache, modulation, w_qkv, qk_gain, output_weight, text_len, refresh):
    batch, img_rows, width_loc = img.shape
    txt_rows = txt.shape[1]
    rows = txt_rows + img_rows
    joined = jnp.concatenate([txt, img], axis=1)
    local_mods = modulation.astype(jnp.float32)
    wide, wide_mod = (
        lax.all_gather(joined, "tp", axis=2, tiled=True),
        lax.all_gather(modulation, "tp", axis=2, tiled=True),
    )
    wide_mods = wide_mod.astype(jnp.float32)
    values = wide.astype(jnp.float32)
    center = jnp.mean(values, axis=2, keepdims=True)
    spread = jnp.mean(jnp.square(values - center), axis=2, keepdims=True)
    normed = (values - center) * lax.rsqrt(spread + EPS)
    modded = (normed * (1.0 + wide_mods[1][:, None, :]) + wide_mods[0][:, None, :]).astype(
        jnp.bfloat16
    )
    offset = lax.axis_index("tp") * width_loc
    own_image = lax.dynamic_slice_in_dim(modded[:, txt_rows:, :], offset, width_loc, 2)
    previous = prev_mod.astype(jnp.float32)
    gap = jnp.sum(jnp.abs(own_image.astype(jnp.float32) - previous), axis=(1, 2))
    base_sum = jnp.sum(jnp.abs(previous), axis=(1, 2))
    numer, denom = lax.psum((gap, base_sum), ("seq", "tp"))
    rel_l1 = numer / jnp.maximum(denom, 1.0)
    columns = w_qkv.shape[2]
    projected = jnp.einsum(
        "btd,dkc->btkc",
        modded,
        lax.all_gather(w_qkv, "seq", axis=0, tiled=True),
        preferred_element_type=jnp.float32,
    )
    heads = columns // HD
    query = unit_heads(projected[:, txt_rows:, 0, :], qk_gain[0]).astype(jnp.bfloat16)
    query_heads = query.reshape(batch, img_rows, heads, HD)
    keyed = unit_heads(projected[:, :, 1, :], qk_gain[1]).astype(jnp.bfloat16)
    valued = projected[:, :, 2, :].astype(jnp.bfloat16)
    paired = jnp.stack([keyed, valued], axis=2)
    score_scale = 1.0 / HD**0.5
    start_top = jnp.full((batch, heads, img_rows), NEG, jnp.float32)
    piece = lax.all_gather(paired, "seq", axis=1, tiled=True)
    top = start_top
    count = piece.shape[1]
    index = jnp.arange(count, dtype=jnp.int32)
    slot = index % rows
    text_pos = index // rows * txt_rows + slot
    valid = (slot >= txt_rows)[None, :] | (text_pos[None, :] < text_len[:, None])
    keys = piece[:, :, 0, :].reshape(batch, count, heads, HD)
    vals = piece[:, :, 1, :].reshape(batch, count, heads, HD)
    logit_scores = (
        jnp.einsum("bqhc,bkhc->bhqk", query_heads, keys, preferred_element_type=jnp.float32)
        * score_scale
    )
    logit_scores = jnp.where(valid[:, None, None, :], logit_scores, NEG)
    new_top = jnp.maximum(top, jnp.max(logit_scores, axis=3))
    attention_weights = jnp.where(
        valid[:, None, None, :], jnp.exp(logit_scores - new_top[..., None]), 0.0
    )
    total = jnp.sum(attention_weights, axis=3)
    summed_output = jnp.einsum(
        "bhqk,bkhc->bhqc",
        attention_weights.astype(jnp.bfloat16),
        vals,
        preferred_element_type=jnp.float32,
    )
    top, total, summed_output = (new_top, total, summed_output)
    attended_values = (summed_output / total[..., None]).astype(jnp.bfloat16)
    attended_values = attended_values.transpose(0, 2, 1, 3).reshape(batch, img_rows, columns)
    partial_output = jnp.einsum(
        "pxr,ro->pxo", attended_values, output_weight, preferred_element_type=jnp.float32
    )
    whole = lax.psum(partial_output.astype(jnp.bfloat16), "tp").astype(jnp.float32)
    mixed_heads = lax.dynamic_slice_in_dim(whole, lax.axis_index("tp") * width_loc, width_loc, 2)
    resid = local_mods[2][:, None, :] * mixed_heads
    flag = (refresh == 1)[:, None, None]
    new_cache = jnp.where(flag, resid, cache)
    out_img = img.astype(jnp.float32) + new_cache
    return (out_img, new_cache, rel_l1)


def head_kernel(n, dims, img_ref, txt_ref, w_ref, wout_ref, gain_ref, lens_ref, rel_ref, mixed_ref, relsum_ref,
                xbuf, wbuf, woutbuf, qbuf, kvbuf, attsrc, attcat, pbuf, rbuf, relbuf,
                local_sem, zsend, ssend, fsend, xrecv, diag_recv, wsend, wrecv, wfsend,
                kvsend, kvrecv, asend, arecv, psend, precv, rsend, rrecv, gbuf, gsend, grecv):
    seq, tp, hloc, cols, half_img, txt_rows, groups = dims
    planes = seq // cols
    me = lax.axis_index("seq")
    t = lax.axis_index("tp")
    other = 1 - t
    z = me // cols
    col = me % cols
    xp = me + 1 - 2 * (me % 2)
    yp = me + 2 - 4 * ((me // 2) % 2)
    rows, width = xbuf.shape[1:]
    half = width // 2
    text = n * half_img
    depth = w_ref.shape[1]

    barrier = pltpu.get_barrier_semaphore()

    def greet(k, carry):
        peer = lax.rem(me * tp + t + k, seq * tp)
        pl.semaphore_signal(barrier, inc=1, device_id=(peer // tp, peer % tp), device_id_type=MESH)
        return carry

    lax.fori_loop(1, seq * tp, greet, 0)

    own = pltpu.make_async_copy(img_ref.at[pl.ds(0, text)], xbuf.at[me, pl.ds(0, text)], local_sem.at[0])
    own.start()
    own_text = pltpu.make_async_copy(txt_ref, xbuf.at[me, pl.ds(text, rows - text)], local_sem.at[2])
    own_text.start()
    wout_copy = pltpu.make_async_copy(wout_ref, woutbuf, local_sem.at[1])
    wout_copy.start()
    pl.semaphore_wait(barrier, seq * tp - 1)

    def remote(src, dst, send, recv, device):
        return pltpu.make_async_remote_copy(
            src_ref=src, dst_ref=dst, send_sem=send, recv_sem=recv,
            device_id=device, device_id_type=MESH,
        )

    def arrived(dst, recv):
        remote(dst, dst, zsend.at[0], recv, (me, other)).wait_recv()

    pending = []

    def launch(copy):
        copy.start()
        pending.append(copy)

    gains = remote(gain_ref, gbuf, gsend.at[0], grecv.at[0], (me, other))
    launch(gains)

    own.wait()
    own_text.wait()
    for dz in range(1, planes):
        there = lax.rem(z + dz, planes) * cols + col
        launch(remote(xbuf.at[me], xbuf.at[me], zsend.at[dz - 1], xrecv.at[me], (there, t)))
    launch(remote(xbuf.at[me], xbuf.at[me], ssend.at[0, 0], xrecv.at[me], (xp, t)))
    launch(remote(xbuf.at[me], xbuf.at[me], ssend.at[0, 1], xrecv.at[me], (yp, t)))

    wcore = me % 2
    for k in range(hloc):
        hl = lax.rem(me + k, hloc)
        head = t * hloc + hl
        same = jnp.logical_and(head == me, wcore == t)

        @pl.when(same)
        def _():
            pltpu.make_async_copy(w_ref.at[:, :, pl.ds(pl.multiple_of(hl * HD, HD), HD)], wbuf.at[me], wrecv.at[me]).start()

        @pl.when(jnp.logical_not(same))
        def _():
            remote(w_ref.at[:, :, pl.ds(pl.multiple_of(hl * HD, HD), HD)], wbuf.at[me], wsend.at[k], wrecv.at[me], (head, wcore)).start()

    for dz in range(1, planes):
        src = lax.rem(z + dz, planes) * cols + col
        arrived(xbuf.at[src], xrecv.at[src])
        launch(remote(xbuf.at[src], xbuf.at[src], ssend.at[dz, 0], xrecv.at[src], (xp, t)))
        launch(remote(xbuf.at[src], xbuf.at[src], ssend.at[dz, 1], xrecv.at[src], (yp, t)))

    for dz in range(planes):
        plane = lax.rem(z + dz, planes)
        sx = plane * cols + xp % cols
        sy = plane * cols + yp % cols
        arrived(xbuf.at[sx], xrecv.at[sx])
        launch(remote(xbuf.at[sx, :, pl.ds(0, half)], xbuf.at[sx, :, pl.ds(0, half)], fsend.at[dz, 0], diag_recv.at[plane, 0], (yp, t)))
        arrived(xbuf.at[sy], xrecv.at[sy])
        launch(remote(xbuf.at[sy, :, pl.ds(half, half)], xbuf.at[sy, :, pl.ds(half, half)], fsend.at[dz, 1], diag_recv.at[plane, 1], (xp, t)))

    for k in range(seq // 2):
        slot = 2 * k + t
        arrived(wbuf.at[slot], wrecv.at[slot])
        launch(remote(wbuf.at[slot], wbuf.at[slot], wfsend.at[k], wrecv.at[slot], (me, other)))

    def send_rel(k, carry):
        peer = lax.rem(me * tp + t + k, seq * tp)
        remote(rel_ref, relbuf.at[me * tp + t], rsend.at[k], rrecv.at[me * tp + t],
               (peer // tp, peer % tp)).start()
        return carry

    lax.fori_loop(1, seq * tp, send_rel, 0)

    for k in range(seq // 2):
        slot = 2 * k + other
        arrived(wbuf.at[slot], wrecv.at[slot])
    for plane in range(planes):
        sd = plane * cols + cols - 1 - col
        for side in range(2):
            arrived(xbuf.at[sd, :, pl.ds(side * half, half)], diag_recv.at[plane, side])

    per = seq // groups
    home = me // hloc
    hl = me % hloc
    head_cols = pl.ds(pl.multiple_of(hl * HD, HD), HD)
    gains.wait_recv()
    gain = jnp.where(home == t, gain_ref[:, head_cols], gbuf[:, head_cols])
    gq, gk = gain[0:1, :], gain[1:2, :]
    weight = jnp.concatenate([wbuf[:, j].reshape(seq * depth, HD) for j in range(3)], axis=1)

    def unit(block, gain):
        return (block * lax.rsqrt(jnp.mean(jnp.square(block), axis=1, keepdims=True) + EPS) * gain).astype(jnp.bfloat16)

    def kv_copy(g):
        part = kvbuf.at[t, pl.ds(g * per, per)]
        return remote(part, part, kvsend.at[g], kvrecv.at[g], (me, other))

    for g in range(groups):
        s0 = g * per
        total = jnp.dot(xbuf[s0:s0 + per].reshape(per * rows, width), weight, preferred_element_type=jnp.float32)
        q = unit(total[:, :HD], gq)
        qbuf[s0:s0 + per] = q.reshape(per, rows, HD)
        k = unit(total[:, HD:2 * HD], gk)
        v = total[:, 2 * HD:].astype(jnp.bfloat16)
        kvbuf[t, s0:s0 + per, 0] = k.reshape(per, rows, HD)
        kvbuf[t, s0:s0 + per, 1] = v.reshape(per, rows, HD)
        launch(kv_copy(g))
    for g in range(groups):
        part = kvbuf.at[other, pl.ds(g * per, per)]
        arrived(part, kvrecv.at[g])

    pad = rows - text
    half_txt = txt_rows // tp
    spot = lax.broadcasted_iota(jnp.int32, (1, tp * seq * pad), 1)
    line = spot % pad
    place = ((spot // pad) % seq) * txt_rows + (spot // (pad * seq)) * half_txt + line % half_txt
    place = place.astype(jnp.float32)
    slot_of = line // half_txt
    always = jnp.ones((1, seq * half_img), jnp.float32)
    for i in range(n):
        lo, hi = i * half_img, (i + 1) * half_img

        def keys(kind):
            parts = [kvbuf[c, :, kind, lo:hi, :].reshape(seq * half_img, HD) for c in range(2)]
            parts += [kvbuf[c, :, kind, text:, :].reshape(seq * pad, HD) for c in range(2)]
            return jnp.concatenate(parts, axis=0)

        q = qbuf[:, lo:hi, :].reshape(seq * half_img, HD)
        scores = lax.dot_general(q, keys(0), (((1,), (1,)), ((), ())),
                                 preferred_element_type=jnp.float32) * (1.0 / HD**0.5)
        seen = jnp.where((slot_of == i) & (place < lens_ref[i:i + 1, 0:1]), 1.0, 0.0)
        valid = jnp.concatenate([always, always, seen], axis=1) > 0.0
        scores = jnp.where(valid, scores, NEG)
        top = jnp.max(scores, axis=1, keepdims=True)
        weights = jnp.where(valid, jnp.exp(scores - top), 0.0)
        total = jnp.sum(weights, axis=1, keepdims=True)
        summed = jnp.dot(weights.astype(jnp.bfloat16), keys(1), preferred_element_type=jnp.float32)
        attsrc[:, lo:hi, :] = (summed / total).astype(jnp.bfloat16).reshape(seq, half_img, HD)

    mine = attcat.at[pl.ds(pl.multiple_of(t * text, half_img), text), pl.ds(pl.multiple_of(hl * HD, HD), HD)]
    for k in range(seq):
        s = lax.rem(me + k, seq)
        if k == 0:
            same = home == t

            @pl.when(same)
            def _():
                pltpu.make_async_copy(attsrc.at[s], mine, arecv.at[hl * 2 + t]).start()

            @pl.when(jnp.logical_not(same))
            def _():
                remote(attsrc.at[s], mine, asend.at[k], arecv.at[hl * 2 + t], (s, home)).start()
        else:
            launch(remote(attsrc.at[s], mine, asend.at[k], arecv.at[hl * 2 + t], (s, home)))
    wout_copy.wait()
    for h in range(hloc):
        for c in range(2):
            arrived(attcat.at[pl.ds(c * text, text), pl.ds(h * HD, HD)], arecv.at[h * 2 + c])

    out_width = mixed_ref.shape[1]
    acts = attcat[...]
    theirs = jnp.dot(acts, woutbuf[:, pl.ds(pl.multiple_of(other * out_width, 128), out_width)],
                     preferred_element_type=jnp.float32)
    pbuf[...] = theirs.astype(jnp.bfloat16)
    give = remote(pbuf, rbuf, psend.at[0], precv.at[0], (me, other))
    launch(give)
    ours = jnp.dot(acts, woutbuf[:, pl.ds(pl.multiple_of(t * out_width, 128), out_width)],
                   preferred_element_type=jnp.float32)

    relbuf[me * tp + t] = rel_ref[...]

    def wait_rel(k, carry):
        peer = lax.rem(me * tp + t + k, seq * tp)
        arrived(relbuf.at[peer], rrecv.at[peer])
        remote(rel_ref, relbuf.at[me * tp + t], rsend.at[k], rrecv.at[me * tp + t],
               (peer // tp, peer % tp)).wait_send()
        return carry

    lax.fori_loop(1, seq * tp, wait_rel, 0)
    relsum_ref[...] = jnp.sum(relbuf[...], axis=0)

    give.wait_recv()
    mixed_ref[...] = ours + rbuf[...].astype(jnp.float32)

    for copy in pending:
        copy.wait_send()
    for k in range(hloc):
        hl_k = lax.rem(me + k, hloc)
        same_k = jnp.logical_and(t * hloc + hl_k == me, wcore == t)

        @pl.when(jnp.logical_not(same_k))
        def _():
            remote(w_ref.at[:, :, pl.ds(pl.multiple_of(hl_k * HD, HD), HD)], wbuf.at[me], wsend.at[k], wrecv.at[me], (t * hloc + hl_k, wcore)).wait_send()

    @pl.when(home != t)
    def _():
        remote(attsrc.at[me], mine, asend.at[0], arecv.at[hl * 2 + t], (me, home)).wait_send()


def head_call(n, seq, tp, half_img, txt_rows, cid, image, text, w_parts, wout, gain, lens, rel):
    cols = 4
    planes = seq // cols
    groups = 4
    _, depth, columns = w_parts.shape
    hloc = columns // HD
    rows, width = n * half_img + text.shape[0], text.shape[1]
    dims = (seq, tp, hloc, cols, half_img, txt_rows, groups)
    out_rows, out_width = n * half_img * tp, wout.shape[1] // tp
    dma = pltpu.SemaphoreType.DMA
    bf16 = jnp.bfloat16
    vmem = pl.BlockSpec(memory_space=pltpu.VMEM)
    hbm = pl.BlockSpec(memory_space=pl.ANY)
    return pl.pallas_call(
        functools.partial(head_kernel, n, dims),
        out_shape=(
            jax.ShapeDtypeStruct((out_rows, out_width), jnp.float32),
            jax.ShapeDtypeStruct(rel.shape, jnp.float32),
        ),
        in_specs=[vmem, vmem, hbm, hbm, vmem, vmem, vmem],
        out_specs=(vmem, vmem),
        scratch_shapes=[
            pltpu.VMEM((seq, rows, width), bf16),
            pltpu.VMEM((seq, 3, depth, HD), bf16),
            pltpu.VMEM(wout.shape, bf16),
            pltpu.VMEM((seq, rows, HD), bf16),
            pltpu.VMEM((tp, seq, 2, rows, HD), bf16),
            pltpu.VMEM((seq, n * half_img, HD), bf16),
            pltpu.VMEM((out_rows, hloc * HD), bf16),
            pltpu.VMEM((out_rows, out_width), bf16),
            pltpu.VMEM((out_rows, out_width), bf16),
            pltpu.VMEM((seq * tp,) + rel.shape, jnp.float32),
            dma((3,)),
            dma((planes,)),
            dma((planes, 2)),
            dma((planes, 2)),
            dma((seq,)),
            dma((planes, 2)),
            dma((hloc,)),
            dma((seq,)),
            dma((seq // 2,)),
            dma((groups,)),
            dma((groups,)),
            dma((seq,)),
            dma((seq,)),
            dma((1,)),
            dma((1,)),
            dma((seq * tp,)),
            dma((seq * tp,)),
            pltpu.VMEM(gain.shape, jnp.float32),
            dma((1,)),
            dma((1,)),
        ],
        compiler_params=pltpu.CompilerParams(
            collective_id=cid, has_side_effects=True, vmem_limit_bytes=58 * 1024 * 1024
        ),
    )(image, text, w_parts, wout, gain, lens, rel)


def by_heads(seq, tp, img, txt, prev_mod, cache, modulation, w_qkv, qk_gain, output_weight, text_len, refresh):
    batch, img_rows, width_loc = img.shape
    txt_rows = txt.shape[1]
    t = lax.axis_index("tp")
    rows_all = txt_rows + img_rows
    local_mods = modulation.astype(jnp.float32)
    joined = jnp.concatenate([txt, img, modulation.transpose(1, 0, 2)], axis=1)
    everything = lax.all_gather(joined, "tp", axis=2, tiled=True)
    wide, wide_mods = everything[:, :rows_all], everything[:, rows_all:].astype(jnp.float32).transpose(1, 0, 2)
    values = wide.astype(jnp.float32)
    center = jnp.mean(values, axis=2, keepdims=True)
    spread = jnp.mean(jnp.square(values - center), axis=2, keepdims=True)
    scale = lax.rsqrt(spread + EPS)

    def modulate(block, mid, inv, mods):
        return ((block - mid) * inv * (1.0 + mods[1][:, None, :]) + mods[0][:, None, :]).astype(jnp.bfloat16)

    own_image = modulate(img.astype(jnp.float32), center[:, txt_rows:], scale[:, txt_rows:], local_mods)
    previous = prev_mod.astype(jnp.float32)
    gap = jnp.sum(jnp.abs(own_image.astype(jnp.float32) - previous), axis=(1, 2))
    base_sum = jnp.sum(jnp.abs(previous), axis=(1, 2))
    rel = jnp.broadcast_to(jnp.stack([gap, base_sum]).reshape(2 * batch, 1), (2 * batch, 128))

    on = refresh == 1
    turn = jnp.arange(batch, dtype=jnp.int32)
    rank = jnp.sum(jnp.where((turn[None, :] < turn[:, None]) & on[None, :], 1, 0), axis=1)
    half_img, half_txt = img_rows // tp, txt_rows // tp
    most = batch - 1
    hit = on[None, :] & (rank[None, :] == jnp.arange(most, dtype=jnp.int32)[:, None])

    def pick(a):
        taken = a[batch - 1][None]
        for b in range(batch - 1):
            taken = jnp.where(hit[:, b, None, None], a[b][None], taken)
        return taken

    def own_rows(start, size):
        cut = lambda a: lax.dynamic_slice_in_dim(a, start, size, 1)
        block = modulate(cut(values), cut(center), cut(scale), wide_mods)
        return pick(block).reshape(most * size, -1)

    image = own_rows(txt_rows + t * half_img, half_img)
    text = own_rows(t * half_txt, half_txt)
    text = jnp.pad(text, ((0, -most * half_txt % 8), (0, 0)))
    lens = jnp.sum(jnp.where(hit, text_len[None, :], 0), axis=1).astype(jnp.float32)
    lens = jnp.broadcast_to(lens[:, None], (most, 128))
    w_parts = w_qkv.transpose(1, 0, 2)

    def run(n, cid):
        mixed, sums = head_call(
            n, seq, tp, half_img, txt_rows, cid, image, text, w_parts, output_weight, qk_gain, lens, rel)
        mixed = mixed.reshape(tp, n, half_img, width_loc).transpose(1, 0, 2, 3).reshape(n, img_rows, width_loc)
        whole = mixed[n - 1][None]
        for k in range(n - 1):
            whole = jnp.where((rank == k)[:, None, None], mixed[k][None], whole)
        return jnp.broadcast_to(whole, img.shape), sums

    level = jnp.clip(jnp.sum(on.astype(jnp.int32)) - 1, 0, batch - 2)
    whole, sums = lax.switch(level, [functools.partial(run, k + 1, k) for k in range(batch - 1)])
    resid = local_mods[2][:, None, :] * whole
    new_cache = jnp.where(on[:, None, None], resid, cache)
    out_img = img.astype(jnp.float32) + new_cache
    numer, denom = sums[:batch, 0], sums[batch:, 0]
    return out_img, new_cache, numer / jnp.maximum(denom, 1.0)


def solution(mesh):
    seq, tp = mesh.shape["seq"], mesh.shape["tp"]

    def step(*args):
        img, txt, w_qkv = args[0], args[1], args[5]
        hloc = w_qkv.shape[2] // HD
        fits = (
            tp == 2 and seq % 8 == 0 and hloc * tp == seq and img.shape[0] == 4
            and img.shape[1] % 32 == 0 and txt.shape[1] % 2 == 0
        )
        if fits:
            return by_heads(seq, tp, *args)
        return local(*args)

    return jax.shard_map(
        step,
        mesh=mesh,
        in_specs=(
            P(None, "seq", "tp"),
            P(None, "seq", "tp"),
            P(None, "seq", "tp"),
            P(None, "seq", "tp"),
            P(None, None, "tp"),
            P("seq", None, "tp"),
            P(None, "tp"),
            P("tp", None),
            P(),
            P(),
        ),
        out_specs=(P(None, "seq", "tp"), P(None, "seq", "tp"), P()),
        check_vma=False,
    )
```

```python
import functools

import jax
import jax.numpy as jnp
from jax import lax
from jax.experimental import pallas as pl
from jax.experimental.pallas import tpu as pltpu
from jax.sharding import PartitionSpec as P

HD = 128
MESH = pl.DeviceIdType.MESH


EPS = 0.1
NEG = -1e30


def unit_heads(block, gain):
    shaped = block.reshape(block.shape[:-1] + (block.shape[-1] // HD, HD))
    scaled = shaped * lax.rsqrt(jnp.mean(jnp.square(shaped), axis=-1, keepdims=True) + EPS)
    return scaled.reshape(block.shape) * gain


def local(img, txt, prev_mod, cache, modulation, w_qkv, qk_gain, output_weight, text_len, refresh):
    batch, img_rows, width_loc = img.shape
    txt_rows = txt.shape[1]
    rows = txt_rows + img_rows
    joined = jnp.concatenate([txt, img], axis=1)
    local_mods = modulation.astype(jnp.float32)
    wide, wide_mod = (
        lax.all_gather(joined, "tp", axis=2, tiled=True),
        lax.all_gather(modulation, "tp", axis=2, tiled=True),
    )
    wide_mods = wide_mod.astype(jnp.float32)
    values = wide.astype(jnp.float32)
    center = jnp.mean(values, axis=2, keepdims=True)
    spread = jnp.mean(jnp.square(values - center), axis=2, keepdims=True)
    normed = (values - center) * lax.rsqrt(spread + EPS)
    modded = (normed * (1.0 + wide_mods[1][:, None, :]) + wide_mods[0][:, None, :]).astype(
        jnp.bfloat16
    )
    offset = lax.axis_index("tp") * width_loc
    own_image = lax.dynamic_slice_in_dim(modded[:, txt_rows:, :], offset, width_loc, 2)
    previous = prev_mod.astype(jnp.float32)
    gap = jnp.sum(jnp.abs(own_image.astype(jnp.float32) - previous), axis=(1, 2))
    base_sum = jnp.sum(jnp.abs(previous), axis=(1, 2))
    numer, denom = lax.psum((gap, base_sum), ("seq", "tp"))
    rel_l1 = numer / jnp.maximum(denom, 1.0)
    columns = w_qkv.shape[2]
    projected = jnp.einsum(
        "btd,dkc->btkc",
        modded,
        lax.all_gather(w_qkv, "seq", axis=0, tiled=True),
        preferred_element_type=jnp.float32,
    )
    heads = columns // HD
    query = unit_heads(projected[:, txt_rows:, 0, :], qk_gain[0]).astype(jnp.bfloat16)
    query_heads = query.reshape(batch, img_rows, heads, HD)
    keyed = unit_heads(projected[:, :, 1, :], qk_gain[1]).astype(jnp.bfloat16)
    valued = projected[:, :, 2, :].astype(jnp.bfloat16)
    paired = jnp.stack([keyed, valued], axis=2)
    score_scale = 1.0 / HD**0.5
    start_top = jnp.full((batch, heads, img_rows), NEG, jnp.float32)
    piece = lax.all_gather(paired, "seq", axis=1, tiled=True)
    top = start_top
    count = piece.shape[1]
    index = jnp.arange(count, dtype=jnp.int32)
    slot = index % rows
    text_pos = index // rows * txt_rows + slot
    valid = (slot >= txt_rows)[None, :] | (text_pos[None, :] < text_len[:, None])
    keys = piece[:, :, 0, :].reshape(batch, count, heads, HD)
    vals = piece[:, :, 1, :].reshape(batch, count, heads, HD)
    logit_scores = (
        jnp.einsum("bqhc,bkhc->bhqk", query_heads, keys, preferred_element_type=jnp.float32)
        * score_scale
    )
    logit_scores = jnp.where(valid[:, None, None, :], logit_scores, NEG)
    new_top = jnp.maximum(top, jnp.max(logit_scores, axis=3))
    attention_weights = jnp.where(
        valid[:, None, None, :], jnp.exp(logit_scores - new_top[..., None]), 0.0
    )
    total = jnp.sum(attention_weights, axis=3)
    summed_output = jnp.einsum(
        "bhqk,bkhc->bhqc",
        attention_weights.astype(jnp.bfloat16),
        vals,
        preferred_element_type=jnp.float32,
    )
    top, total, summed_output = (new_top, total, summed_output)
    attended_values = (summed_output / total[..., None]).astype(jnp.bfloat16)
    attended_values = attended_values.transpose(0, 2, 1, 3).reshape(batch, img_rows, columns)
    partial_output = jnp.einsum(
        "pxr,ro->pxo", attended_values, output_weight, preferred_element_type=jnp.float32
    )
    whole = lax.psum(partial_output.astype(jnp.bfloat16), "tp").astype(jnp.float32)
    mixed_heads = lax.dynamic_slice_in_dim(whole, lax.axis_index("tp") * width_loc, width_loc, 2)
    resid = local_mods[2][:, None, :] * mixed_heads
    flag = (refresh == 1)[:, None, None]
    new_cache = jnp.where(flag, resid, cache)
    out_img = img.astype(jnp.float32) + new_cache
    return (out_img, new_cache, rel_l1)


def head_kernel(n, dims, refresh_ref, len_ref, img_ref, txt_ref, prev_ref, mod_ref, w_ref, wout_ref, gain_ref, mixed_ref, relsum_ref,
                xbuf, wbuf, woutbuf, qbuf, kvbuf, attsrc, attcat, pbuf, rbuf, relbuf,
                local_sem, zsend, ssend, fsend, xrecv, diag_recv, wsend, wrecv, wfsend,
                kvsend, kvrecv, asend, arecv, psend, precv, rsend, rrecv, gbuf, pimg, ptxt, pmod, img_mod, txt_mod, relsrc, gsend, grecv):
    seq, tp, hloc, cols, half_img, txt_rows, groups = dims
    planes = seq // cols
    me = lax.axis_index("seq")
    t = lax.axis_index("tp")
    other = 1 - t
    z = me // cols
    col = me % cols
    xp = me + 1 - 2 * (me % 2)
    yp = me + 2 - 4 * ((me // 2) % 2)
    rows, width = xbuf.shape[1:]
    half = width // 2
    text = n * half_img
    depth = w_ref.shape[1]

    barrier = pltpu.get_barrier_semaphore()

    def greet(k, carry):
        peer = lax.rem(me * tp + t + k, seq * tp)
        pl.semaphore_signal(barrier, inc=1, device_id=(peer // tp, peer % tp), device_id_type=MESH)
        return carry

    lax.fori_loop(1, seq * tp, greet, 0)

    wout_copy = pltpu.make_async_copy(wout_ref, woutbuf, local_sem.at[1])
    wout_copy.start()
    pl.semaphore_wait(barrier, seq * tp - 1)

    def remote(src, dst, send, recv, device):
        return pltpu.make_async_remote_copy(
            src_ref=src, dst_ref=dst, send_sem=send, recv_sem=recv,
            device_id=device, device_id_type=MESH,
        )

    def arrived(dst, recv):
        remote(dst, dst, zsend.at[0], recv, (me, other)).wait_recv()

    pending = []

    def launch(copy):
        copy.start()
        pending.append(copy)

    swaps = [
        remote(img_ref, pimg, gsend.at[1], grecv.at[1], (me, other)),
        remote(txt_ref, ptxt, gsend.at[2], grecv.at[2], (me, other)),
        remote(mod_ref, pmod, gsend.at[3], grecv.at[3], (me, other)),
    ]
    for swap in swaps:
        launch(swap)
    gains = remote(gain_ref, gbuf, gsend.at[0], grecv.at[0], (me, other))
    launch(gains)

    wcore = me % 2
    early = 3

    def send_weights(k):
        hl = lax.rem(me + k, hloc)
        head = t * hloc + hl
        same = jnp.logical_and(head == me, wcore == t)

        @pl.when(same)
        def _():
            pltpu.make_async_copy(w_ref.at[:, :, pl.ds(pl.multiple_of(hl * HD, HD), HD)], wbuf.at[me], wrecv.at[me]).start()

        @pl.when(jnp.logical_not(same))
        def _():
            remote(w_ref.at[:, :, pl.ds(pl.multiple_of(hl * HD, HD), HD)], wbuf.at[me], wsend.at[k], wrecv.at[me], (head, wcore)).start()

    for k in range(early):
        send_weights(k)

    batch = img_ref.shape[0]
    slots = []
    for i in range(n):
        pick, rank = jnp.int32(0), jnp.int32(0)
        for b in range(batch):
            on = jnp.where(refresh_ref[b] == 1, 1, 0)
            pick = pick + jnp.where(rank == i, on, 0) * b
            rank = rank + on
        slots.append(pick)
    for swap in swaps:
        swap.wait_recv()
    mine_mod = mod_ref[...].astype(jnp.float32)
    their_mod = pmod[...].astype(jnp.float32)
    rel_rows = []

    def modulate(a, p, b):
        mid = (jnp.sum(a, axis=1, keepdims=True) + jnp.sum(p, axis=1, keepdims=True)) / width
        a, p = a - mid, p - mid
        spread = (jnp.sum(a * a, axis=1, keepdims=True) + jnp.sum(p * p, axis=1, keepdims=True)) / width
        inv = lax.rsqrt(spread + EPS)
        a = a * inv * (1.0 + mine_mod[1, b:b + 1]) + mine_mod[0, b:b + 1]
        p = p * inv * (1.0 + their_mod[1, b:b + 1]) + their_mod[0, b:b + 1]
        return a.astype(jnp.bfloat16), p.astype(jnp.bfloat16)

    bases = []
    for b in range(batch):
        a, p = modulate(img_ref[b].astype(jnp.float32), pimg[b].astype(jnp.float32), b)
        img_mod[t, b] = a
        img_mod[other, b] = p
        previous = prev_ref[b].astype(jnp.float32)
        rel_rows.append(jnp.sum(jnp.abs(a.astype(jnp.float32) - previous), keepdims=True))
        bases.append(jnp.sum(jnp.abs(previous), keepdims=True))
        a, p = modulate(txt_ref[b].astype(jnp.float32), ptxt[b].astype(jnp.float32), b)
        txt_mod[t, b] = a.astype(jnp.float32)
        txt_mod[other, b] = p.astype(jnp.float32)
    relsrc[...] = jnp.concatenate([jnp.broadcast_to(row, (1, 128)) for row in rel_rows + bases], axis=0)
    half_txt = txt_rows // tp
    pad = rows - text
    for side in range(2):
        for i in range(n):
            xbuf[me, i * half_img:(i + 1) * half_img, side * half:(side + 1) * half] = img_mod[
                side, slots[i], pl.ds(pl.multiple_of(t * half_img, half_img), half_img), :]
        pieces = []
        for i in range(n):
            block = txt_mod[side, slots[i]]
            pieces.append(jnp.where(t == 0, block[:half_txt], block[half_txt:]))
        if pad > n * half_txt:
            pieces.append(jnp.zeros((pad - n * half_txt, half), jnp.float32))
        xbuf[me, text:rows, side * half:(side + 1) * half] = jnp.concatenate(pieces, axis=0).astype(jnp.bfloat16)

    for dz in range(1, planes):
        there = lax.rem(z + dz, planes) * cols + col
        launch(remote(xbuf.at[me], xbuf.at[me], zsend.at[dz - 1], xrecv.at[me], (there, t)))
    launch(remote(xbuf.at[me], xbuf.at[me], ssend.at[0, 0], xrecv.at[me], (xp, t)))
    launch(remote(xbuf.at[me], xbuf.at[me], ssend.at[0, 1], xrecv.at[me], (yp, t)))

    for k in range(early, hloc):
        send_weights(k)

    for dz in range(1, planes):
        src = lax.rem(z + dz, planes) * cols + col
        arrived(xbuf.at[src], xrecv.at[src])
        launch(remote(xbuf.at[src], xbuf.at[src], ssend.at[dz, 0], xrecv.at[src], (xp, t)))
        launch(remote(xbuf.at[src], xbuf.at[src], ssend.at[dz, 1], xrecv.at[src], (yp, t)))

    for dz in range(planes):
        plane = lax.rem(z + dz, planes)
        sx = plane * cols + xp % cols
        sy = plane * cols + yp % cols
        arrived(xbuf.at[sx], xrecv.at[sx])
        launch(remote(xbuf.at[sx, :, pl.ds(0, half)], xbuf.at[sx, :, pl.ds(0, half)], fsend.at[dz, 0], diag_recv.at[plane, 0], (yp, t)))
        arrived(xbuf.at[sy], xrecv.at[sy])
        launch(remote(xbuf.at[sy, :, pl.ds(half, half)], xbuf.at[sy, :, pl.ds(half, half)], fsend.at[dz, 1], diag_recv.at[plane, 1], (xp, t)))

    for k in range(seq // 2):
        slot = 2 * k + t
        arrived(wbuf.at[slot], wrecv.at[slot])
        launch(remote(wbuf.at[slot], wbuf.at[slot], wfsend.at[k], wrecv.at[slot], (me, other)))

    def send_rel(k, carry):
        peer = lax.rem(me * tp + t + k, seq * tp)
        remote(relsrc, relbuf.at[me * tp + t], rsend.at[k], rrecv.at[me * tp + t],
               (peer // tp, peer % tp)).start()
        return carry

    lax.fori_loop(1, seq * tp, send_rel, 0)

    for k in range(seq // 2):
        slot = 2 * k + other
        arrived(wbuf.at[slot], wrecv.at[slot])
    for plane in range(planes):
        sd = plane * cols + cols - 1 - col
        for side in range(2):
            arrived(xbuf.at[sd, :, pl.ds(side * half, half)], diag_recv.at[plane, side])

    per = seq // groups
    home = me // hloc
    hl = me % hloc
    head_cols = pl.ds(pl.multiple_of(hl * HD, HD), HD)
    gains.wait_recv()
    gain = jnp.where(home == t, gain_ref[:, head_cols], gbuf[:, head_cols])
    gq, gk = gain[0:1, :], gain[1:2, :]
    weight = jnp.concatenate([wbuf[:, j].reshape(seq * depth, HD) for j in range(3)], axis=1)

    def unit(block, gain):
        return (block * lax.rsqrt(jnp.mean(jnp.square(block), axis=1, keepdims=True) + EPS) * gain).astype(jnp.bfloat16)

    def kv_copy(g):
        part = kvbuf.at[t, pl.ds(g * per, per)]
        return remote(part, part, kvsend.at[g], kvrecv.at[g], (me, other))

    for g in range(groups):
        s0 = g * per
        total = jnp.dot(xbuf[s0:s0 + per].reshape(per * rows, width), weight, preferred_element_type=jnp.float32)
        q = unit(total[:, :HD], gq)
        qbuf[s0:s0 + per] = q.reshape(per, rows, HD)
        k = unit(total[:, HD:2 * HD], gk)
        v = total[:, 2 * HD:].astype(jnp.bfloat16)
        kvbuf[t, s0:s0 + per, 0] = k.reshape(per, rows, HD)
        kvbuf[t, s0:s0 + per, 1] = v.reshape(per, rows, HD)
        launch(kv_copy(g))
    for g in range(groups):
        part = kvbuf.at[other, pl.ds(g * per, per)]
        arrived(part, kvrecv.at[g])

    spot = lax.broadcasted_iota(jnp.int32, (1, tp * seq * pad), 1)
    line = spot % pad
    place = ((spot // pad) % seq) * txt_rows + (spot // (pad * seq)) * half_txt + line % half_txt
    slot_of = line // half_txt
    always = jnp.ones((1, seq * half_img), jnp.float32)
    for i in range(n):
        lo, hi = i * half_img, (i + 1) * half_img

        def keys(kind):
            parts = [kvbuf[c, :, kind, lo:hi, :].reshape(seq * half_img, HD) for c in range(2)]
            parts += [kvbuf[c, :, kind, text:, :].reshape(seq * pad, HD) for c in range(2)]
            return jnp.concatenate(parts, axis=0)

        q = qbuf[:, lo:hi, :].reshape(seq * half_img, HD)
        scores = lax.dot_general(q, keys(0), (((1,), (1,)), ((), ())),
                                 preferred_element_type=jnp.float32) * (1.0 / HD**0.5)
        seen = jnp.where((slot_of == i) & (place < len_ref[slots[i]]), 1.0, 0.0)
        valid = jnp.concatenate([always, always, seen], axis=1) > 0.0
        scores = jnp.where(valid, scores, NEG)
        top = jnp.max(scores, axis=1, keepdims=True)
        weights = jnp.where(valid, jnp.exp(scores - top), 0.0)
        total = jnp.sum(weights, axis=1, keepdims=True)
        summed = jnp.dot(weights.astype(jnp.bfloat16), keys(1), preferred_element_type=jnp.float32)
        attsrc[:, lo:hi, :] = (summed / total).astype(jnp.bfloat16).reshape(seq, half_img, HD)

    mine = attcat.at[pl.ds(pl.multiple_of(t * text, half_img), text), pl.ds(pl.multiple_of(hl * HD, HD), HD)]
    for k in range(seq):
        s = lax.rem(me + k, seq)
        if k == 0:
            same = home == t

            @pl.when(same)
            def _():
                pltpu.make_async_copy(attsrc.at[s], mine, arecv.at[hl * 2 + t]).start()

            @pl.when(jnp.logical_not(same))
            def _():
                remote(attsrc.at[s], mine, asend.at[k], arecv.at[hl * 2 + t], (s, home)).start()
        else:
            launch(remote(attsrc.at[s], mine, asend.at[k], arecv.at[hl * 2 + t], (s, home)))
    wout_copy.wait()
    for h in range(hloc):
        for c in range(2):
            arrived(attcat.at[pl.ds(c * text, text), pl.ds(h * HD, HD)], arecv.at[h * 2 + c])

    out_width = mixed_ref.shape[1]
    acts = attcat[...]
    theirs = jnp.dot(acts, woutbuf[:, pl.ds(pl.multiple_of(other * out_width, 128), out_width)],
                     preferred_element_type=jnp.float32)
    pbuf[...] = theirs.astype(jnp.bfloat16)
    give = remote(pbuf, rbuf, psend.at[0], precv.at[0], (me, other))
    launch(give)
    ours = jnp.dot(acts, woutbuf[:, pl.ds(pl.multiple_of(t * out_width, 128), out_width)],
                   preferred_element_type=jnp.float32)

    relbuf[me * tp + t] = relsrc[...]

    def wait_rel(k, carry):
        peer = lax.rem(me * tp + t + k, seq * tp)
        arrived(relbuf.at[peer], rrecv.at[peer])
        remote(relsrc, relbuf.at[me * tp + t], rsend.at[k], rrecv.at[me * tp + t],
               (peer // tp, peer % tp)).wait_send()
        return carry

    lax.fori_loop(1, seq * tp, wait_rel, 0)
    relsum_ref[...] = jnp.sum(relbuf[...], axis=0)

    give.wait_recv()
    mixed_ref[...] = ours + rbuf[...].astype(jnp.float32)

    for copy in pending:
        copy.wait_send()
    for k in range(hloc):
        hl_k = lax.rem(me + k, hloc)
        same_k = jnp.logical_and(t * hloc + hl_k == me, wcore == t)

        @pl.when(jnp.logical_not(same_k))
        def _():
            remote(w_ref.at[:, :, pl.ds(pl.multiple_of(hl_k * HD, HD), HD)], wbuf.at[me], wsend.at[k], wrecv.at[me], (t * hloc + hl_k, wcore)).wait_send()

    @pl.when(home != t)
    def _():
        remote(attsrc.at[me], mine, asend.at[0], arecv.at[hl * 2 + t], (me, home)).wait_send()


def head_call(n, seq, tp, cid, refresh, text_len, img, txt, prev_mod, modulation, w_parts, wout, gain):
    cols = 4
    planes = seq // cols
    groups = 4
    _, depth, columns = w_parts.shape
    hloc = columns // HD
    batch, img_rows, half = img.shape
    txt_rows = txt.shape[1]
    half_img = img_rows // tp
    rows, width = n * half_img - (-n * (txt_rows // tp) // 8) * 8, half * tp
    rel_shape = (2 * batch, 128)
    dims = (seq, tp, hloc, cols, half_img, txt_rows, groups)
    out_rows, out_width = n * half_img * tp, wout.shape[1] // tp
    dma = pltpu.SemaphoreType.DMA
    bf16 = jnp.bfloat16
    vmem = pl.BlockSpec(memory_space=pltpu.VMEM)
    smem = pl.BlockSpec(memory_space=pltpu.SMEM)
    hbm = pl.BlockSpec(memory_space=pl.ANY)
    return pl.pallas_call(
        functools.partial(head_kernel, n, dims),
        out_shape=(
            jax.ShapeDtypeStruct((out_rows, out_width), jnp.float32),
            jax.ShapeDtypeStruct(rel_shape, jnp.float32),
        ),
        in_specs=[smem, smem, vmem, vmem, vmem, vmem, hbm, hbm, vmem],
        out_specs=(vmem, vmem),
        scratch_shapes=[
            pltpu.VMEM((seq, rows, width), bf16),
            pltpu.VMEM((seq, 3, depth, HD), bf16),
            pltpu.VMEM(wout.shape, bf16),
            pltpu.VMEM((seq, rows, HD), bf16),
            pltpu.VMEM((tp, seq, 2, rows, HD), bf16),
            pltpu.VMEM((seq, n * half_img, HD), bf16),
            pltpu.VMEM((out_rows, hloc * HD), bf16),
            pltpu.VMEM((out_rows, out_width), bf16),
            pltpu.VMEM((out_rows, out_width), bf16),
            pltpu.VMEM((seq * tp,) + rel_shape, jnp.float32),
            dma((3,)),
            dma((planes,)),
            dma((planes, 2)),
            dma((planes, 2)),
            dma((seq,)),
            dma((planes, 2)),
            dma((hloc,)),
            dma((seq,)),
            dma((seq // 2,)),
            dma((groups,)),
            dma((groups,)),
            dma((seq,)),
            dma((seq,)),
            dma((1,)),
            dma((1,)),
            dma((seq * tp,)),
            dma((seq * tp,)),
            pltpu.VMEM(gain.shape, jnp.float32),
            pltpu.VMEM(img.shape, bf16),
            pltpu.VMEM(txt.shape, bf16),
            pltpu.VMEM(modulation.shape, bf16),
            pltpu.VMEM((tp,) + img.shape, bf16),
            pltpu.VMEM((tp,) + txt.shape, jnp.float32),
            pltpu.VMEM(rel_shape, jnp.float32),
            dma((4,)),
            dma((4,)),
        ],
        compiler_params=pltpu.CompilerParams(
            collective_id=cid, has_side_effects=True, vmem_limit_bytes=58 * 1024 * 1024
        ),
    )(refresh, text_len, img, txt, prev_mod, modulation, w_parts, wout, gain)


def by_heads(seq, tp, img, txt, prev_mod, cache, modulation, w_qkv, qk_gain, output_weight, text_len, refresh):
    batch, img_rows, width_loc = img.shape
    local_mods = modulation.astype(jnp.float32)
    on = refresh == 1
    turn = jnp.arange(batch, dtype=jnp.int32)
    rank = jnp.sum(jnp.where((turn[None, :] < turn[:, None]) & on[None, :], 1, 0), axis=1)
    half_img = img_rows // tp
    w_parts = w_qkv.transpose(1, 0, 2)

    def run(n, cid):
        mixed, sums = head_call(
            n, seq, tp, cid, refresh, text_len, img, txt, prev_mod, modulation, w_parts, output_weight, qk_gain)
        mixed = mixed.reshape(tp, n, half_img, width_loc).transpose(1, 0, 2, 3).reshape(n, img_rows, width_loc)
        whole = mixed[n - 1][None]
        for k in range(n - 1):
            whole = jnp.where((rank == k)[:, None, None], mixed[k][None], whole)
        return jnp.broadcast_to(whole, img.shape), sums

    level = jnp.clip(jnp.sum(on.astype(jnp.int32)) - 1, 0, batch - 2)
    whole, sums = lax.switch(level, [functools.partial(run, k + 1, k) for k in range(batch - 1)])
    resid = local_mods[2][:, None, :] * whole
    new_cache = jnp.where(on[:, None, None], resid, cache)
    out_img = img.astype(jnp.float32) + new_cache
    numer, denom = sums[:batch, 0], sums[batch:, 0]
    return out_img, new_cache, numer / jnp.maximum(denom, 1.0)


def solution(mesh):
    seq, tp = mesh.shape["seq"], mesh.shape["tp"]

    def step(*args):
        img, txt, w_qkv = args[0], args[1], args[5]
        hloc = w_qkv.shape[2] // HD
        fits = (
            tp == 2 and seq % 8 == 0 and hloc * tp == seq and img.shape[0] == 4
            and img.shape[1] % 32 == 0 and txt.shape[1] % 2 == 0
        )
        if fits:
            return by_heads(seq, tp, *args)
        return local(*args)

    return jax.shard_map(
        step,
        mesh=mesh,
        in_specs=(
            P(None, "seq", "tp"),
            P(None, "seq", "tp"),
            P(None, "seq", "tp"),
            P(None, "seq", "tp"),
            P(None, None, "tp"),
            P("seq", None, "tp"),
            P(None, "tp"),
            P("tp", None),
            P(),
            P(),
        ),
        out_specs=(P(None, "seq", "tp"), P(None, "seq", "tp"), P()),
        check_vma=False,
    )
```
